64 devices in a mesh: dp: 4 (over x, y), cp: 16 (over z, core).
Axes of the slice: x: 2, y: 2, z: 8, core: 2. Of those that a mesh axis runs over, the one named last changes fastest.
The devices are a block of a 4x4x8 slice.
Arguments:
- x: bfloat16 [32768, 2560], P(('dp', 'cp')), parts along dimension 0
- g: bfloat16 [6, 2560], replicated
- wq: bfloat16 [6, 2560, 8, 256], replicated
- wk: bfloat16 [6, 2560, 4, 256], replicated
- wv: bfloat16 [6, 2560, 4, 256], replicated
- wo: bfloat16 [6, 8, 256, 2560], replicated
Outputs:
- output: bfloat16 [32768, 2560], P(('dp', 'cp')), parts along dimension 0
There are 4 independent parts. The reference program is written for one: setup_inputs(seed, part) draws one part's arguments, and reference() takes and returns one part's arrays. A program takes and returns all parts, laid end to end along the dimension named above; an argument that names none is the same for every part.
All inputs are finite; a program needn't handle non-finite values.
Results may differ from the reference program's by a relative error of at most 0.02.
Values are sent between devices in bfloat16 or wider.
A program may use at most 768 MiB of HBM per device.

```python
import numpy as np
import jax
import jax.numpy as jnp
from jax import lax

CP = 16
S = 8192
D = 2560
HQ = 8
HKV = 4
DH = 256
W = 1024
L_LOC = 5

EPS = 1e-6
R = S // (2 * CP)
QB = min(256, R)
NL = L_LOC + 1


def _layout():
    runs = np.stack([np.arange(CP), 2 * CP - 1 - np.arange(CP)], axis=1).reshape(-1)
    return (runs[:, None] * R + np.arange(R)[None, :]).reshape(-1)


def setup_inputs(seed: int = 0, part: int = 0) -> dict:
    key = jax.random.PRNGKey(seed)
    kx = jax.random.fold_in(jax.random.fold_in(key, 1), part)
    kg, kq, kk, kv, ko = jax.random.split(jax.random.fold_in(key, 2), 5)
    x = 0.5 * jax.random.normal(kx, (S, D), jnp.float32)
    g = 1.0 + 0.2 * jax.random.normal(kg, (NL, D), jnp.float32)
    wq = 1.5 * D ** -0.5 * jax.random.normal(kq, (NL, D, HQ, DH), jnp.float32)
    wk = 1.5 * D ** -0.5 * jax.random.normal(kk, (NL, D, HKV, DH), jnp.float32)
    wv = D ** -0.5 * jax.random.normal(kv, (NL, D, HKV, DH), jnp.float32)
    wo = (HQ * DH) ** -0.5 * jax.random.normal(ko, (NL, HQ, DH, D), jnp.float32)
    return {'x': x.astype(jnp.bfloat16), 'g': g.astype(jnp.bfloat16), 'wq': wq.astype(jnp.bfloat16),
            'wk': wk.astype(jnp.bfloat16), 'wv': wv.astype(jnp.bfloat16), 'wo': wo.astype(jnp.bfloat16)}


def _rms(x, g):
    xf = x.astype(jnp.float32)
    n = xf * lax.rsqrt(jnp.mean(xf * xf, axis=-1, keepdims=True) + EPS)
    return (n * g.astype(jnp.float32)).astype(jnp.bfloat16)


def _attend(q, k, v, qp, kp, local):
    s = jnp.einsum('qhgd,khd->hgqk', q.astype(jnp.float32), k.astype(jnp.float32)) * DH ** -0.5
    ok = (kp[None, :] <= qp[:, None]) & (kp[None, :] >= 0)
    if local:
        ok = ok & (kp[None, :] > qp[:, None] - W)
    s = jnp.where(ok, s, -jnp.inf)
    p = jax.nn.softmax(s, axis=-1).astype(jnp.bfloat16)
    o = jnp.einsum('hgqk,khd->qhgd', p.astype(jnp.float32), v.astype(jnp.float32))
    return o.astype(jnp.bfloat16)


def _layer(x, g, wq, wk, wv, wo, local):
    n = _rms(x, g)
    q = jnp.dot(n, wq.reshape(D, HQ * DH), preferred_element_type=jnp.float32).astype(jnp.bfloat16)
    q = q.reshape(S, HKV, HQ // HKV, DH)
    k = jnp.dot(n, wk.reshape(D, HKV * DH), preferred_element_type=jnp.float32).astype(jnp.bfloat16).reshape(S, HKV, DH)
    v = jnp.dot(n, wv.reshape(D, HKV * DH), preferred_element_type=jnp.float32).astype(jnp.bfloat16).reshape(S, HKV, DH)
    if local:
        zeros = jnp.zeros((W, HKV, DH), jnp.bfloat16)
        kk = jnp.concatenate([zeros, k])
        vv = jnp.concatenate([zeros, v])
        kp = jnp.arange(S + W) - W
    else:
        kk, vv, kp = k, v, jnp.arange(S)
    nk = W + QB

    def blk(t0):
        qs = lax.dynamic_slice_in_dim(q, t0, QB)
        qp = t0 + jnp.arange(QB)
        if local:
            return _attend(qs, lax.dynamic_slice_in_dim(kk, t0, nk), lax.dynamic_slice_in_dim(vv, t0, nk),
                           qp, lax.dynamic_slice_in_dim(kp, t0, nk), True)
        return _attend(qs, kk, vv, qp, kp, False)

    o = lax.map(blk, jnp.arange(S // QB) * QB).reshape(S, HQ * DH)
    y = jnp.dot(o, wo.reshape(HQ * DH, D), preferred_element_type=jnp.float32)
    return (x.astype(jnp.float32) + y).astype(jnp.bfloat16)


def reference(x, g, wq, wk, wv, wo):
    idx = _layout()
    inv = np.argsort(idx)
    h = x[inv]
    for l in range(NL):
        h = _layer(h, g[l], wq[l], wk[l], wv[l], wo[l], l < L_LOC)
    return h[idx]
```

```python
import functools
import math

import jax
import jax.numpy as jnp
from jax import lax
from jax.experimental import pallas as pl
from jax.experimental.pallas import tpu as pltpu
from jax.sharding import PartitionSpec as P

W = 1024
EPS = 1e-6
F32 = jnp.float32
BF16 = jnp.bfloat16
MESH = pl.DeviceIdType.MESH
CHUNKS = 8
SLOTS = 3
NEG = float('-inf')


def _dot(a, b):
    return jnp.dot(a, b, preferred_element_type=F32)


def _dot_nt(a, b):
    return lax.dot_general(a, b, (((1,), (1,)), ((), ())), preferred_element_type=F32)


def _for(n, body):
    lax.fori_loop(0, n, lambda j, c: (body(j), c)[1], 0)


def _barrier(cp, i, partner):
    sem = pltpu.get_barrier_semaphore()
    for nb in (lax.rem(i + 2, cp), lax.rem(i + cp - 2, cp), partner):
        pl.semaphore_signal(sem, inc=1, device_id={'cp': nb}, device_id_type=MESH)
    pl.semaphore_wait(sem, 3)


def _remote(src, dst, ssem, rsem, dev):
    return pltpu.make_async_remote_copy(src_ref=src, dst_ref=dst, send_sem=ssem, recv_sem=rsem,
                                        device_id={'cp': dev}, device_id_type=MESH)


def _norm(x, n, g):
    rows = 64 if x.shape[0] % 64 == 0 else x.shape[0]

    def blk(j):
        sl = pl.ds(pl.multiple_of(j * rows, rows), rows)
        v = x[sl, :]
        s = lax.rsqrt(jnp.mean(v * v, axis=-1, keepdims=True) + EPS)
        n[sl, :] = (v * s * g).astype(BF16)

    _for(x.shape[0] // rows, blk)


def _round_rows(x, dst):
    rows = 64 if x.shape[0] % 64 == 0 else x.shape[0]

    def blk(j):
        sl = pl.ds(pl.multiple_of(j * rows, rows), rows)
        v = x[sl, :].astype(BF16)
        if dst is None:
            x[sl, :] = v.astype(F32)
        else:
            dst[sl, :] = v

    _for(x.shape[0] // rows, blk)


def _load_rows(src, x):
    rows = 64 if x.shape[0] % 64 == 0 else x.shape[0]

    def blk(j):
        sl = pl.ds(pl.multiple_of(j * rows, rows), rows)
        x[sl, :] = src[sl, :].astype(F32)

    _for(x.shape[0] // rows, blk)


def _out_proj(x, o, wo, slot):
    d = x.shape[1]
    nb = min(512, d)

    def blk(j):
        sl = pl.ds(pl.multiple_of(j * nb, nb), nb)
        x[:, sl] += _dot(o[...], wo[slot, :, sl])

    _for(d // nb, blk)


def _local_kernel(cp, nloc, x_hbm, g_ref, wq_hbm, wk_hbm, wv_hbm, wo_hbm, xo_hbm, wkvo_hbm, wqo_hbm,
                  x, n, q, wkv, wq, wo, own, halo, stage, o, pq, pkv,
                  msem, ssem, wosem, send, extra, recv):
    t, d = x.shape
    r = t // 2
    hkv, dh = own.shape[0] // 2, own.shape[2] // 2
    nz = cp // 2
    i = lax.axis_index('cp')
    c = lax.rem(i, 2)
    z = lax.div(i, 2)
    partner = i + 1 - 2 * c
    last = z == nz - 1
    crows = stage.shape[1]
    nblk = crows // 256
    scale = dh ** -0.5 * math.log2(math.e)

    def yes():
        return z >= 0

    cc = (c, 1 - c)
    nxt_dev = (lax.rem(i + 2, cp), lax.rem(i + cp - 2, cp))
    nxt = (z + 1 < nz, z > 0)
    e2 = (z >= 1, yes())
    e4 = (z >= 2, yes())

    def hidx(par, s, p, h):
        return ((par * 2 + s) * 4 + p) * hkv + h

    def hs(par, s, p, h):
        return halo.at[hidx(par, s, p, h)]

    def copy(kind, s, h, par):
        ownr = own.at[s * hkv + h]
        sem = send.at[(kind * 2 + s) * hkv + h]
        if kind == 0:
            src, p, dev = ownr, 1, nxt_dev[s]
        elif kind == 1:
            src, p, dev = hs(par, s, 1, h), 3, nxt_dev[s]
        elif kind == 2:
            src, p, dev = ownr, 0, partner
        elif kind == 3:
            src, p, dev = hs(par, s, 1, h), 0, partner
        elif kind == 4:
            src, p, dev = hs(par, s, 1, h), 2, partner
        else:
            src, p, dev = hs(par, s, 3, h), 2, partner
        return _remote(src, hs(par, s, p, h), sem, recv.at[hidx(par, s, p, h)], dev)

    def cond(kind, s):
        lead, follow = cc[s] == 0, cc[s] == 1
        return (nxt[s], nxt[s] & e2[s], lead, follow & e2[s], lead & e2[s], follow & e4[s])[kind]

    def start(kind, s, h, par):
        pl.when(cond(kind, s))(lambda: copy(kind, s, h, par).start())

    def edge_copy(h, par):
        return _remote(own.at[h], hs(par, 1, 1, h), extra.at[h], recv.at[hidx(par, 1, 1, h)], partner)

    def edge_local(p, h, par):
        return pltpu.make_async_copy(hs(par, 0, p, h), hs(par, 1, 3, h), recv.at[hidx(par, 1, 3, h)])

    def arrived(s, p, h, par, when):
        slot = hs(par, s, p, h)
        pl.when(when)(lambda: pltpu.make_async_copy(slot, slot, recv.at[hidx(par, s, p, h)]).wait())

    def raw(kv, l, j):
        sl = pl.ds(pl.multiple_of(j * crows, 256), crows)
        slot = lax.rem(j, SLOTS)
        if kv:
            return (pltpu.make_async_copy(wk_hbm.at[l, sl], stage.at[slot, :, pl.ds(0, 128)], ssem.at[slot]),
                    pltpu.make_async_copy(wv_hbm.at[l, sl], stage.at[slot, :, pl.ds(128, 128)], ssem.at[SLOTS + slot]))
        return (pltpu.make_async_copy(wq_hbm.at[l, sl], stage.at[slot], ssem.at[slot]),)

    def prefetch(kv, l):
        for j in range(SLOTS):
            for cpy in raw(kv, l, j):
                cpy.start()

    def relayout(kv, l):
        unroll = 5 if nblk % 5 == 0 else 1

        def chunk(j):
            for cpy in raw(kv, l, j):
                cpy.wait()
            slot = lax.rem(j, SLOTS)

            def group(b):
                for u in range(unroll):
                    bb = b * unroll + u
                    blk = stage[slot, pl.ds(pl.multiple_of(bb * 256, 256), 256), :]
                    out = _dot(pkv[...] if kv else pq[...], blk).astype(BF16)
                    rows = pl.ds(pl.multiple_of((j * nblk + bb) * 32, 32), 32)
                    for a in range(8):
                        part = out[a * 32:(a + 1) * 32]
                        if kv:
                            h, lane = a // 2, (a % 2) * 128
                            wkv[h, rows, lane:lane + 128] = part[:, :128]
                            wkv[h, rows, dh + lane:dh + lane + 128] = part[:, 128:]
                        else:
                            wq[a // 2, rows, (a % 2) * dh:(a % 2 + 1) * dh] = part

            _for(nblk // unroll, group)

            @pl.when(j + SLOTS < CHUNKS)
            def _():
                for cpy in raw(kv, l, j + SLOTS):
                    cpy.start()

        _for(CHUNKS, chunk)

    def wo_copy(l, h):
        slot = lax.rem(h, 2)
        return pltpu.make_async_copy(wo_hbm.at[l, pl.ds(pl.multiple_of(h * 2 * dh, 2 * dh), 2 * dh)], wo.at[slot], wosem.at[slot])

    load_x = pltpu.make_async_copy(x_hbm, n, msem.at[0])
    load_x.start()
    prefetch(True, 0)
    wo_copy(0, 0).start()
    wo_copy(0, 1).start()

    @pl.when(z < 2)
    def _():
        def clear(j):
            par = lax.div(j, 4 * hkv)
            halo[par * 8 * hkv + lax.rem(j, 4 * hkv)] = jnp.zeros(halo.shape[1:], BF16)

        _for(8 * hkv, clear)

    _barrier(cp, i, partner)
    ro = lax.broadcasted_iota(jnp.int32, (256, 256), 0)
    co = lax.broadcasted_iota(jnp.int32, (256, 256), 1)
    pq[...] = jnp.where(co == (ro % 32) * 8 + ro // 32, 1.0, 0.0).astype(BF16)
    pkv[...] = jnp.where(co == (ro % 32) * 8 + ((ro // 32) % 2) * 4 + ro // 64, 1.0, 0.0).astype(BF16)
    relayout(True, 0)
    prefetch(False, 0)
    load_x.wait()
    _load_rows(n, x)
    _norm(x, n, g_ref[0])

    rows = lax.broadcasted_iota(jnp.int32, (2 * r, r), 0) % r
    cols = lax.broadcasted_iota(jnp.int32, (2 * r, r), 1)

    def attend(s, h, par):
        qv = q[s * hkv + h]
        ks = [own[s * hkv + h, :, :dh]] + [halo[hidx(par, s, p, h), :, :dh] for p in range(4)]
        vs = [own[s * hkv + h, :, dh:]] + [halo[hidx(par, s, p, h), :, dh:] for p in range(4)]
        sc = [_dot_nt(qv, k) for k in ks]
        sc[0] = jnp.where(cols <= rows, sc[0], NEG)
        sc[4] = jnp.where(cols > rows, sc[4], NEG)
        if s == 0:
            for b in range(1, 5):
                sc[b] = sc[b] + jnp.where(i >= b, 0.0, NEG).astype(F32)
        m = functools.reduce(jnp.maximum, sc).max(axis=1, keepdims=True)
        pr = [jnp.exp2((v - m) * scale) for v in sc]
        den = functools.reduce(jnp.add, pr).sum(axis=1, keepdims=True)
        num = functools.reduce(jnp.add, [_dot(a.astype(BF16), v) for a, v in zip(pr, vs)])
        out = (num / den).astype(BF16)
        o[s * r:(s + 1) * r, :dh] = out[:r]
        o[s * r:(s + 1) * r, dh:] = out[r:]

    def layer(l):
        par = lax.rem(l, 2)

        def kv_head(h):
            y = _dot(n[...], wkv[h]).astype(BF16)
            own[h] = y[:r]
            own[hkv + h] = y[r:]
            for s in range(2):
                start(0, s, h, par)
                start(2, s, h, par)
            pl.when(last)(lambda: edge_copy(h, par).start())

        _for(hkv, kv_head)

        @pl.when(l == 0)
        def _():
            relayout(False, 0)
        prefetch(True, l + 1)

        def q_group(h):
            y = _dot(n[...], wq[h]).astype(BF16)
            for s in range(2):
                q[s * hkv + h, :r] = y[s * r:(s + 1) * r, :dh]
                q[s * hkv + h, r:] = y[s * r:(s + 1) * r, dh:]

        _for(hkv, q_group)

        def forward(h):
            for s in range(2):
                arrived(s, 1, h, par, e2[s])
                for kind in (1, 3, 4):
                    start(kind, s, h, par)

        forward(0)
        relayout(True, l + 1)
        prefetch(False, l + 1)
        forward(1)
        relayout(False, l + 1)
        forward(2)
        forward(3)

        def head(h):
            arrived(0, 3, h, par, e4[0])
            start(5, 0, h, par)
            arrived(0, 0, h, par, (c == 1) | e2[0])
            arrived(0, 2, h, par, jnp.where(c == 1, z >= 1, z >= 2))
            pl.when(last & (c == 1))(lambda: edge_local(2, h, par).start())
            pl.when(last & (c == 0))(lambda: edge_local(0, h, par).start())
            arrived(1, 3, h, par, yes())
            start(5, 1, h, par)
            arrived(1, 0, h, par, yes())
            arrived(1, 2, h, par, yes())
            attend(0, h, par)
            attend(1, h, par)
            wo_copy(l, h).wait()
            _out_proj(x, o, wo, lax.rem(h, 2))

            @pl.when((h < hkv - 2) | (l < nloc - 1))
            def _():
                wrap = lax.div(h + 2, hkv)
                wo_copy(l + wrap, h + 2 - hkv * wrap).start()

        _for(hkv, head)

        def drain(h):
            for s in range(2):
                for kind in range(6):
                    pl.when(cond(kind, s))(lambda k=kind, s=s: copy(k, s, h, par).wait_send())
            pl.when(last)(lambda: edge_copy(h, par).wait_send())

        _for(hkv, drain)

        @pl.when(l < nloc - 1)
        def _():
            _round_rows(x, None)
            _norm(x, n, g_ref[l + 1])

    _for(nloc, layer)
    out_kv = pltpu.make_async_copy(wkv, wkvo_hbm, msem.at[1])
    out_q = pltpu.make_async_copy(wq, wqo_hbm, msem.at[2])
    out_kv.start()
    out_q.start()
    _round_rows(x, n)
    out_x = pltpu.make_async_copy(n, xo_hbm, msem.at[0])
    out_x.start()
    out_kv.wait()
    out_q.wait()
    out_x.wait()


def _global_kernel(cp, lay, x_hbm, g_ref, wkv_hbm, wq_hbm, wo_hbm, y_hbm,
                   x, q, kvg, acc, mx, den, wst, wo, o,
                   msem, wsem, wosem, isend, irecv, dsend, drecv):
    t, d = x.shape
    r = t // 2
    hkv, dh = q.shape[0] // 2, q.shape[2]
    nz = cp // 2
    i = lax.axis_index('cp')
    c = lax.rem(i, 2)
    z = lax.div(i, 2)
    partner = i + 1 - 2 * c
    scale = dh ** -0.5 * math.log2(math.e)
    nxt_dev = (lax.rem(i + 2, cp), lax.rem(i + cp - 2, cp))

    def run_of(s, k, core):
        if s == 0:
            return lax.rem(z - k + nz, nz) * 2 + core
        return 2 * cp - 1 - (z + k) * 2 - core

    def slot(s, k, core, h):
        return run_of(s, k, core) * hkv + h

    def has(s, k):
        return (k < nz) if s == 0 else (z + k < nz)

    def sends(s, k):
        return (k < nz - 1) if s == 0 else ((z + k < nz) & (z > 0))

    def sidx(s, k, h):
        return (s * nz + k) * hkv + h

    def ici(s, k, h):
        ref = kvg.at[slot(s, k, c, h)]
        return _remote(ref, ref, isend.at[sidx(s, k, h)], irecv.at[sidx(s, k + 1, h)], nxt_dev[s])

    def d2d(s, k, h):
        ref = kvg.at[slot(s, k, c, h)]
        return _remote(ref, ref, dsend.at[sidx(s, k, h)], drecv.at[sidx(s, k, h)], partner)

    def push(s, k, h):
        pl.when(sends(s, k))(lambda: ici(s, k, h).start())
        pl.when(has(s, k))(lambda: d2d(s, k, h).start())

    def got_ici(s, k, h):
        ref = kvg.at[slot(s, k, c, h)]
        pl.when(has(s, k))(lambda: pltpu.make_async_copy(ref, ref, irecv.at[sidx(s, k, h)]).wait())

    def got_d2d(s, k, h):
        ref = kvg.at[slot(s, k, 1 - c, h)]
        pl.when(has(s, k))(lambda: pltpu.make_async_copy(ref, ref, drecv.at[sidx(s, k, h)]).wait())

    def wtile(j):
        src = wkv_hbm.at[j] if j < hkv else wq_hbm.at[j - hkv]
        return pltpu.make_async_copy(src, wst.at[j % 2], wsem.at[j % 2])

    def wo_copy(h):
        sl = lax.rem(h, 2)
        return pltpu.make_async_copy(wo_hbm.at[lay, pl.ds(pl.multiple_of(h * 2 * dh, 2 * dh), 2 * dh)], wo.at[sl], wosem.at[sl])

    load_x = pltpu.make_async_copy(x_hbm, wo.at[0, :t], msem.at[0])
    load_x.start()
    wtile(0).start()
    wtile(1).start()
    _barrier(cp, i, partner)
    load_x.wait()
    n = wo.at[1, :t]
    _load_rows(wo.at[0, :t], x)
    _norm(x, n, g_ref[lay])
    for j in range(2 * hkv):
        wtile(j).wait()
        y = _dot(n[...], wst[j % 2]).astype(BF16)
        if j < hkv:
            kvg[slot(0, 0, c, j)] = y[:r]
            kvg[slot(1, 0, c, j)] = y[r:]
            for s in range(2):
                push(s, 0, j)
        else:
            for s in range(2):
                q[s * hkv + j - hkv, :r] = y[s * r:(s + 1) * r, :dh]
                q[s * hkv + j - hkv, r:] = y[s * r:(s + 1) * r, dh:]
        if j + 2 < 2 * hkv:
            wtile(j + 2).start()
    wo_copy(0).start()
    wo_copy(1).start()

    def init(j):
        acc[j] = jnp.zeros(acc.shape[1:], F32)
        mx[j] = jnp.full(mx.shape[1:], NEG, F32)
        den[j] = jnp.zeros(den.shape[1:], F32)

    _for(2 * hkv, init)
    rows = lax.broadcasted_iota(jnp.int32, (2 * r, r), 0) % r
    cols = lax.broadcasted_iota(jnp.int32, (2 * r, r), 1)

    def flash(qs, ks, k, h, masked):
        qi = qs * hkv + h
        qv = q[qi]
        sl = [slot(ks, k, core, h) for core in range(2)]
        sc = [_dot_nt(qv, kvg[a, :, :dh]) for a in sl]
        if masked:
            rq = run_of(qs, 0, c)
            sc = [jnp.where(cols - rows <= (rq - run_of(ks, k, core)) * r, v, NEG) for core, v in enumerate(sc)]
        old = mx[qi][:, :1]
        m = jnp.maximum(old, jnp.maximum(sc[0], sc[1]).max(axis=1, keepdims=True))
        a = jnp.exp2((old - m) * scale)
        pr = [jnp.exp2((v - m) * scale) for v in sc]
        dn = den[qi][:, :1] * a + (pr[0] + pr[1]).sum(axis=1, keepdims=True)
        acc[qi] = acc[qi] * a + (_dot(pr[0].astype(BF16), kvg[sl[0], :, dh:]) + _dot(pr[1].astype(BF16), kvg[sl[1], :, dh:]))
        mx[qi] = jnp.broadcast_to(m, mx.shape[1:])
        den[qi] = jnp.broadcast_to(dn, den.shape[1:])

    def step(k, h):
        for s in range(2):
            got_d2d(s, k, h)

        def job(j):
            qs = jnp.where(j < 2, 1, 0)
            run0 = jnp.where(j == 1, run_of(1, k, 0), run_of(0, k, 0))
            run1 = jnp.where(j == 1, run_of(1, k, 1), run_of(0, k, 1))
            ok = jnp.where(j == 1, z + k < nz, jnp.where(j == 2, z - k >= 0, z >= 0))
            pl.when(ok)(lambda: flash_at(qs * hkv + h, run0 * hkv + h, run1 * hkv + h))

        _for(3, job)

    def flash_at(qi, s0, s1):
        qv = q[qi]
        sc = [_dot_nt(qv, kvg[a, :, :dh]) for a in (s0, s1)]
        old = mx[qi][:, :1]
        m = jnp.maximum(old, jnp.maximum(sc[0], sc[1]).max(axis=1, keepdims=True))
        a = jnp.exp2((old - m) * scale)
        pr = [jnp.exp2((v - m) * scale) for v in sc]
        dn = den[qi][:, :1] * a + (pr[0] + pr[1]).sum(axis=1, keepdims=True)
        acc[qi] = acc[qi] * a + (_dot(pr[0].astype(BF16), kvg[s0, :, dh:]) + _dot(pr[1].astype(BF16), kvg[s1, :, dh:]))
        mx[qi] = jnp.broadcast_to(m, mx.shape[1:])
        den[qi] = jnp.broadcast_to(dn, den.shape[1:])

    def finish(h):
        for s in range(2):
            qi = s * hkv + h
            out = (acc[qi] / den[qi][:, :1]).astype(BF16)
            o[s * r:(s + 1) * r, :dh] = out[:r]
            o[s * r:(s + 1) * r, dh:] = out[r:]
        wo_copy(h).wait()
        _out_proj(x, o, wo, lax.rem(h, 2))
        pl.when(h + 2 < hkv)(lambda: wo_copy(h + 2).start())

    def main(j):
        k = 1 + lax.div(j, hkv)
        h = lax.rem(j, hkv)
        for s in range(2):
            got_ici(s, k, h)
            push(s, k, h)

        @pl.when(k == 1)
        def _():
            for s in range(2):
                got_d2d(s, 0, h)
            flash(0, 0, 0, h, True)
            flash(1, 0, 0, h, False)
            flash(1, 1, 0, h, True)

        jp = j - 1
        kp = 1 + lax.div(jp, hkv)
        hp = lax.rem(jp, hkv)

        @pl.when(j > 0)
        def _():
            step(kp, hp)
            pl.when(kp == nz - 1)(lambda: finish(hp))

    _for((nz - 1) * hkv, main)
    step(nz - 1, hkv - 1)
    finish(hkv - 1)
    _round_rows(x, wo.at[0, :t])
    out = pltpu.make_async_copy(wo.at[0, :t], y_hbm, msem.at[0])
    out.start()

    def drain(j):
        k = lax.div(j, hkv)
        h = lax.rem(j, hkv)
        for s in range(2):
            pl.when(sends(s, k))(lambda s=s: ici(s, k, h).wait_send())
            pl.when(has(s, k))(lambda s=s: d2d(s, k, h).wait_send())

    _for(nz * hkv, drain)
    out.wait()


def solution(mesh):
    cp = mesh.shape['cp']

    def body(x, g, wq, wk, wv, wo):
        t, d = x.shape
        r = t // 2
        nl = g.shape[0]
        hq, dh = wq.shape[2], wq.shape[3]
        hkv = wk.shape[2]
        assert (hq, hkv, dh, W) == (8, 4, 256, 4 * r)
        gf = g.astype(F32).reshape(nl, 1, d)
        wq2 = wq.reshape(nl, d * hq, dh)
        wk2, wv2 = (a.reshape(nl, d, hkv, 2, dh // 2).transpose(0, 1, 3, 2, 4).reshape(nl, d * hkv * 2, dh // 2) for a in (wk, wv))
        wo2 = wo.reshape(nl, hq * dh, d)
        hbm = pl.BlockSpec(memory_space=pl.ANY)
        vmem = pl.BlockSpec(memory_space=pltpu.VMEM)
        sems = pltpu.SemaphoreType.DMA
        shape = jax.ShapeDtypeStruct
        limit = 67043328
        tile = (hkv, d, 2 * dh)
        x1, wkv_l, wq_l = pl.pallas_call(
            functools.partial(_local_kernel, cp, nl - 1),
            out_shape=(shape((t, d), BF16), shape(tile, BF16), shape(tile, BF16)),
            in_specs=[hbm, vmem, hbm, hbm, hbm, hbm],
            out_specs=(hbm, hbm, hbm),
            scratch_shapes=[
                pltpu.VMEM((t, d), F32),
                pltpu.VMEM((t, d), BF16),
                pltpu.VMEM((2 * hkv, 2 * r, dh), BF16),
                pltpu.VMEM(tile, BF16),
                pltpu.VMEM(tile, BF16),
                pltpu.VMEM((2, 2 * dh, d), BF16),
                pltpu.VMEM((2 * hkv, r, 2 * dh), BF16),
                pltpu.VMEM((2 * 2 * 4 * hkv, r, 2 * dh), BF16),
                pltpu.VMEM((SLOTS, d * hq // CHUNKS, dh), BF16),
                pltpu.VMEM((t, 2 * dh), BF16),
                pltpu.VMEM((256, 256), BF16),
                pltpu.VMEM((256, 256), BF16),
                sems((3,)), sems((2 * SLOTS,)), sems((2,)), sems((6 * 2 * hkv,)), sems((hkv,)), sems((2 * 2 * 4 * hkv,)),
            ],
            compiler_params=pltpu.CompilerParams(collective_id=0, has_side_effects=True, vmem_limit_bytes=limit),
            name='local_layers',
        )(x, gf, wq2, wk2, wv2, wo2)
        nz = cp // 2
        return pl.pallas_call(
            functools.partial(_global_kernel, cp, nl - 1),
            out_shape=shape((t, d), BF16),
            in_specs=[hbm, vmem, hbm, hbm, hbm],
            out_specs=hbm,
            scratch_shapes=[
                pltpu.VMEM((t, d), F32),
                pltpu.VMEM((2 * hkv, 2 * r, dh), BF16),
                pltpu.VMEM((2 * cp * hkv, r, 2 * dh), BF16),
                pltpu.VMEM((2 * hkv, 2 * r, dh), F32),
                pltpu.VMEM((2 * hkv, 2 * r, 128), F32),
                pltpu.VMEM((2 * hkv, 2 * r, 128), F32),
                pltpu.VMEM((2, d, 2 * dh), BF16),
                pltpu.VMEM((2, 2 * dh, d), BF16),
                pltpu.VMEM((t, 2 * dh), BF16),
                sems((1,)), sems((2,)), sems((2,)),
                sems((2 * nz * hkv,)), sems((2 * nz * hkv,)), sems((2 * nz * hkv,)), sems((2 * nz * hkv,)),
            ],
            compiler_params=pltpu.CompilerParams(collective_id=1, has_side_effects=True, vmem_limit_bytes=limit),
            name='global_layer',
        )(x1, gf, wkv_l, wq_l, wo2)

    spec = P(('dp', 'cp'), None)
    return jax.shard_map(body, mesh=mesh, in_specs=(spec, P(), P(), P(), P(), P()), out_specs=spec, check_vma=False)
```

```python
import functools
import math

import jax
import jax.numpy as jnp
from jax import lax
from jax.experimental import pallas as pl
from jax.experimental.pallas import tpu as pltpu
from jax.sharding import PartitionSpec as P

W = 1024
EPS = 1e-6
F32 = jnp.float32
BF16 = jnp.bfloat16
MESH = pl.DeviceIdType.MESH
CHUNKS = 16
SLOTS = 6
NEG = float('-inf')


def _dot(a, b):
    return jnp.dot(a, b, preferred_element_type=F32)


def _dot_nt(a, b):
    return lax.dot_general(a, b, (((1,), (1,)), ((), ())), preferred_element_type=F32)


def _for(n, body):
    lax.fori_loop(0, n, lambda j, c: (body(j), c)[1], 0)


def _barrier(cp, i, partner):
    sem = pltpu.get_barrier_semaphore()
    for nb in (lax.rem(i + 2, cp), lax.rem(i + cp - 2, cp), partner):
        pl.semaphore_signal(sem, inc=1, device_id={'cp': nb}, device_id_type=MESH)
    pl.semaphore_wait(sem, 3)


def _remote(src, dst, ssem, rsem, dev):
    return pltpu.make_async_remote_copy(src_ref=src, dst_ref=dst, send_sem=ssem, recv_sem=rsem,
                                        device_id={'cp': dev}, device_id_type=MESH)


def _blocks(lo, n, body):
    rows = 64

    def blk(j):
        body(pl.ds(pl.multiple_of(lo + j * rows, rows), rows))

    _for(n // rows, blk)


def _norm(x, n, g, lo, cnt):
    def blk(sl):
        v = x[sl, :].astype(BF16).astype(F32)
        x[sl, :] = v
        s = lax.rsqrt(jnp.mean(v * v, axis=-1, keepdims=True) + EPS)
        n[sl, :] = (v * s * g).astype(BF16)

    _blocks(lo, cnt, blk)


def _cast_rows(src, dst):
    def blk(sl):
        dst[sl, :] = src[sl, :].astype(dst.dtype)

    _blocks(0, src.shape[0], blk)


def _turn(eye, a):
    return _dot_nt(eye[...], a).astype(BF16)


def _scores(k, qt):
    return _dot(k.reshape(-1, k.shape[-1]), qt)


def _eye():
    ro = lax.broadcasted_iota(jnp.int32, (256, 256), 0)
    co = lax.broadcasted_iota(jnp.int32, (256, 256), 1)
    return jnp.where(ro == co, 1.0, 0.0).astype(BF16)


def _out_proj(x, lo, o, wo, slot, rows):
    d = x.shape[1]
    nb = min(512, d)
    for j in range(d // nb):
        sl = slice(j * nb, (j + 1) * nb)
        x[lo:lo + rows, sl] += _dot(o[lo:lo + rows, :], wo[slot, :, sl])


def _store_o(eye, o, s, r, ot):
    dh = ot.shape[0]
    ob = ot.astype(BF16)
    for g in range(2):
        o[s * r:(s + 1) * r, g * dh:(g + 1) * dh] = _turn(eye, ob[:, g * r:(g + 1) * r])


def _local_kernel(cp, nloc, x_hbm, g_ref, wq_hbm, wk_hbm, wv_hbm, wo_hbm, xo_hbm, wkvo_hbm, wqo_hbm,
                  x, n, q, wkv, wq, wo, own, near, far, stage, o, pq, pkv,
                  msem, ssem, wosem, send, extra, recv):
    t, d = x.shape
    r = t // 2
    hkv, dh = own.shape[0] // 2, own.shape[2] // 2
    nz = cp // 2
    i = lax.axis_index('cp')
    c = lax.rem(i, 2)
    z = lax.div(i, 2)
    partner = i + 1 - 2 * c
    last = z == nz - 1
    crows = stage.shape[1]
    nblk = crows // 256
    scale = dh ** -0.5 * math.log2(math.e)

    def yes():
        return z >= 0

    cc = (c, 1 - c)
    nxt_dev = (lax.rem(i + 2, cp), lax.rem(i + cp - 2, cp))
    nxt = (z + 1 < nz, z > 0)
    e2 = (z >= 1, yes())
    e4 = (z >= 2, yes())

    def hs(par, s, p, h):
        if p < 2:
            return near.at[((par * 2 + s) * hkv + h) * 2 + p]
        return far.at[(s * hkv + h) * 2 + p - 2]

    def rsem(par, s, p, h):
        return recv.at[((par * 2 + s) * 4 + p) * hkv + h]

    def copy(kind, s, h, par):
        ownr = own.at[s * hkv + h]
        sem = send.at[(kind * 2 + s) * hkv + h]
        if kind == 0:
            src, p, dev = ownr, 1, nxt_dev[s]
        elif kind == 1:
            src, p, dev = hs(par, s, 1, h), 3, nxt_dev[s]
        elif kind == 2:
            src, p, dev = ownr, 0, partner
        elif kind == 3:
            src, p, dev = hs(par, s, 1, h), 0, partner
        elif kind == 4:
            src, p, dev = hs(par, s, 1, h), 2, partner
        else:
            src, p, dev = hs(par, s, 3, h), 2, partner
        return _remote(src, hs(par, s, p, h), sem, rsem(par, s, p, h), dev)

    def cond(kind, s):
        lead, follow = cc[s] == 0, cc[s] == 1
        return (nxt[s], nxt[s] & e2[s], lead, follow & e2[s], lead & e2[s], follow & e4[s])[kind]

    def start(kind, s, h, par):
        pl.when(cond(kind, s))(lambda: copy(kind, s, h, par).start())

    def edge_copy(h, par):
        return _remote(own.at[h], hs(par, 1, 1, h), extra.at[h], rsem(par, 1, 1, h), partner)

    def edge_local(p, h, par):
        return pltpu.make_async_copy(hs(par, 0, p, h), hs(par, 1, 3, h), rsem(par, 1, 3, h))

    def arrived(s, p, h, par, when):
        slot = hs(par, s, p, h)
        pl.when(when)(lambda: pltpu.make_async_copy(slot, slot, rsem(par, s, p, h)).wait())

    def raw(kv, l, j):
        sl = pl.ds(pl.multiple_of(j * crows, 256), crows)
        slot = lax.rem(j, SLOTS)
        if kv:
            return (pltpu.make_async_copy(wk_hbm.at[l, sl], stage.at[slot, :, pl.ds(0, 128)], ssem.at[slot]),
                    pltpu.make_async_copy(wv_hbm.at[l, sl], stage.at[slot, :, pl.ds(128, 128)], ssem.at[SLOTS + slot]))
        return (pltpu.make_async_copy(wq_hbm.at[l, sl], stage.at[slot], ssem.at[slot]),)

    def prefetch(kv, l):
        for j in range(SLOTS):
            for cpy in raw(kv, l, j):
                cpy.start()

    def relayout(kv, l):
        def chunk(j):
            for cpy in raw(kv, l, j):
                cpy.wait()
            slot = lax.rem(j, SLOTS)
            for b in range(nblk):
                blk = stage[slot, b * 256:(b + 1) * 256, :]
                out = _dot(pkv[...] if kv else pq[...], blk).astype(BF16)
                rows = pl.ds(pl.multiple_of((j * nblk + b) * 32, 32), 32)
                for a in range(8):
                    part = out[a * 32:(a + 1) * 32]
                    if kv:
                        h, lane = a // 2, (a % 2) * 128
                        wkv[h, rows, lane:lane + 128] = part[:, :128]
                        wkv[h, rows, dh + lane:dh + lane + 128] = part[:, 128:]
                    else:
                        wq[a // 2, rows, (a % 2) * dh:(a % 2 + 1) * dh] = part

            @pl.when(j + SLOTS < CHUNKS)
            def _():
                for cpy in raw(kv, l, j + SLOTS):
                    cpy.start()

        _for(CHUNKS, chunk)

    def wo_copy(l, h):
        slot = lax.rem(h, 2)
        return pltpu.make_async_copy(wo_hbm.at[l, pl.ds(pl.multiple_of(h * 2 * dh, 2 * dh), 2 * dh)], wo.at[slot], wosem.at[slot])

    load_x = pltpu.make_async_copy(x_hbm, n, msem.at[0])
    prefetch(True, 0)
    load_x.start()

    @pl.when(z < 2)
    def _():
        def clear(j):
            near[lax.div(j, 2 * hkv) * 4 * hkv + lax.rem(j, 2 * hkv)] = jnp.zeros(near.shape[1:], BF16)

        def clear_far(j):
            far[j] = jnp.zeros(far.shape[1:], BF16)

        _for(4 * hkv, clear)
        _for(2 * hkv, clear_far)

    _barrier(cp, i, partner)
    ro = lax.broadcasted_iota(jnp.int32, (256, 256), 0)
    co = lax.broadcasted_iota(jnp.int32, (256, 256), 1)
    pq[...] = jnp.where(co == (ro % 32) * 8 + ro // 32, 1.0, 0.0).astype(BF16)
    pkv[...] = jnp.where(co == (ro % 32) * 8 + ((ro // 32) % 2) * 4 + ro // 64, 1.0, 0.0).astype(BF16)
    rows = lax.broadcasted_iota(jnp.int32, (2 * r, r), 0) % r
    cols = lax.broadcasted_iota(jnp.int32, (2 * r, r), 1)

    def attend(s, h, par):
        qi = s * hkv + h
        qv = q[qi]
        jn = ((par * 2 + s) * hkv + h) * 2
        jf = qi * 2
        sn = _dot_nt(qv, near[pl.ds(jn, 2), :, :dh].reshape(2 * r, dh))
        sf = _dot_nt(qv, far[pl.ds(jf, 2), :, :dh].reshape(2 * r, dh))
        sc = [jnp.where(cols <= rows, _dot_nt(qv, own[qi, :, :dh]), NEG), sn[:, :r], sn[:, r:],
              sf[:, :r], jnp.where(cols > rows, sf[:, r:], NEG)]
        if s == 0:
            for b in range(1, 5):
                sc[b] = sc[b] + jnp.where(i >= b, 0.0, NEG).astype(F32)
        m = functools.reduce(jnp.maximum, sc).max(axis=1, keepdims=True)
        pr = [jnp.exp2((v - m) * scale) for v in sc]
        den = functools.reduce(jnp.add, pr).sum(axis=1, keepdims=True)
        vs = [own[qi, :, dh:], near[jn, :, dh:], near[jn + 1, :, dh:], far[jf, :, dh:], far[jf + 1, :, dh:]]
        num = functools.reduce(jnp.add, [_dot(a.astype(BF16), v) for a, v in zip(pr, vs)])
        out = (num / den).astype(BF16)
        o[s * r:(s + 1) * r, :dh] = out[:r]
        o[s * r:(s + 1) * r, dh:] = out[r:]

    def kv_store(s, h, y):
        own[s * hkv + h] = y

    def kv_send(s, h, par):
        start(0, s, h, par)
        start(2, s, h, par)
        if s == 0:
            pl.when(last)(lambda: edge_copy(h, par).start())

    def kv_first(s, par):
        kv_store(s, 0, _dot(n[s * r:(s + 1) * r, :], wkv[0]).astype(BF16))
        kv_send(s, 0, par)

    def drain(s, h, par):
        for kind in range(6):
            pl.when(cond(kind, s))(lambda k=kind: copy(k, s, h, par).wait_send())
        if s == 0:
            pl.when(last)(lambda: edge_copy(h, par).wait_send())

    relayout(True, 0)
    load_x.wait()
    prefetch(False, 0)
    _cast_rows(n, x)
    for s in range(2):
        _norm(x, n, g_ref[0], s * r, r)
        kv_first(s, 0)
    wo_copy(0, 0).start()
    wo_copy(0, 1).start()

    def layer(l):
        par = lax.rem(l, 2)

        def kv_head(j):
            h = j + 1
            y = _dot(n[...], wkv[h]).astype(BF16)
            for s in range(2):
                kv_store(s, h, y[s * r:(s + 1) * r])
                kv_send(s, h, par)

        _for(hkv - 1, kv_head)

        @pl.when(l == 0)
        def _():
            relayout(False, 0)
        prefetch(True, l + 1)

        def q_group(h):
            y = _dot(n[...], wq[h]).astype(BF16)
            for s in range(2):
                q[s * hkv + h, :r] = y[s * r:(s + 1) * r, :dh]
                q[s * hkv + h, r:] = y[s * r:(s + 1) * r, dh:]

        _for(hkv, q_group)

        def forward(h):
            for s in range(2):
                arrived(s, 1, h, par, e2[s])
                arrived(s, 0, h, par, cc[s] == 1)
            for s in range(2):
                for kind in (1, 3, 4):
                    start(kind, s, h, par)

        forward(0)
        relayout(True, l + 1)
        prefetch(False, l + 1)
        forward(1)
        relayout(False, l + 1)
        forward(2)
        forward(3)

        def far_ready(s, h):
            arrived(s, 0, h, par, (cc[s] == 0) & e2[s])
            arrived(s, 3, h, par, e4[s])
            start(5, s, h, par)

        def far_wait(s, h):
            arrived(s, 2, h, par, jnp.where(cc[0] == 1, z >= 1, z >= 2) if s == 0 else yes())
            if s == 0:
                pl.when(last & (c == 1))(lambda: edge_local(2, h, par).start())
                pl.when(last & (c == 0))(lambda: edge_local(0, h, par).start())

        def next_wo(h):
            @pl.when((h < hkv - 2) | (l < nloc - 1))
            def _():
                wrap = lax.div(h + 2, hkv)
                wo_copy(l + wrap, h + 2 - hkv * wrap).start()

        def head(h):
            far_ready(0, h)
            far_wait(0, h)
            far_ready(1, h)
            far_wait(1, h)
            attend(0, h, par)
            attend(1, h, par)
            wo_copy(l, h).wait()
            _out_proj(x, 0, o, wo, lax.rem(h, 2), t)
            next_wo(h)

        _for(hkv - 1, head)
        h3 = hkv - 1
        wo_copy(l, h3).wait()

        def tail(s):
            far_ready(s, h3)
            far_wait(s, h3)
            attend(s, h3, par)
            _out_proj(x, s * r, o, wo, h3 % 2, r)
            if s == 0:
                _for(hkv - 1, lambda h: (drain(0, h, par), drain(1, h, par)))
            drain(s, h3, par)

            @pl.when(l < nloc - 1)
            def _():
                _norm(x, n, g_ref[l + 1], s * r, r)
                kv_first(s, 1 - par)

        tail(0)
        tail(1)
        next_wo(h3)

    _for(nloc, layer)
    out_kv = pltpu.make_async_copy(wkv, wkvo_hbm, msem.at[1])
    out_q = pltpu.make_async_copy(wq, wqo_hbm, msem.at[2])
    out_kv.start()
    out_q.start()
    _cast_rows(x, n)
    out_x = pltpu.make_async_copy(n, xo_hbm, msem.at[0])
    out_x.start()
    out_kv.wait()
    out_q.wait()
    out_x.wait()


def _global_kernel(cp, lay, x_hbm, g_ref, wkv_hbm, wq_hbm, wo_hbm, y_hbm,
                   x, qt, kvg, acc, ml, wst, wo, o, eye,
                   msem, wsem, wosem, isend, irecv, dsend, drecv):
    t, d = x.shape
    r = t // 2
    hkv, dh = qt.shape[0] // 2, qt.shape[1]
    nz = cp // 2
    i = lax.axis_index('cp')
    c = lax.rem(i, 2)
    z = lax.div(i, 2)
    partner = i + 1 - 2 * c
    scale = dh ** -0.5 * math.log2(math.e)
    nxt_dev = (lax.rem(i + 2, cp), lax.rem(i + cp - 2, cp))

    def pair_of(s, k):
        return lax.rem(z - k + nz, nz) if s == 0 else cp - 1 - (z + k)

    def in_pair(s, core):
        return core if s == 0 else 1 - core

    def slot(s, k, core, h):
        return (pair_of(s, k) * hkv + h) * 2 + in_pair(s, core)

    def has(s, k):
        return (k < nz) if s == 0 else (z + k < nz)

    def sends(s, k):
        return (k < nz - 1) if s == 0 else ((z + k < nz) & (z > 0))

    def sidx(s, k, h):
        return (s * nz + k) * hkv + h

    def ici(s, k, h):
        ref = kvg.at[slot(s, k, c, h)]
        return _remote(ref, ref, isend.at[sidx(s, k, h)], irecv.at[sidx(s, k + 1, h)], nxt_dev[s])

    def d2d(s, k, h):
        ref = kvg.at[slot(s, k, c, h)]
        return _remote(ref, ref, dsend.at[sidx(s, k, h)], drecv.at[sidx(s, k, h)], partner)

    def push(s, k, h):
        pl.when(sends(s, k))(lambda: ici(s, k, h).start())
        pl.when(has(s, k))(lambda: d2d(s, k, h).start())

    def got_ici(s, k, h):
        ref = kvg.at[slot(s, k, c, h)]
        pl.when(has(s, k))(lambda: pltpu.make_async_copy(ref, ref, irecv.at[sidx(s, k, h)]).wait())

    def got_d2d(s, k, h):
        ref = kvg.at[slot(s, k, 1 - c, h)]
        pl.when(has(s, k))(lambda: pltpu.make_async_copy(ref, ref, drecv.at[sidx(s, k, h)]).wait())

    def wtile(j):
        src = wkv_hbm.at[j] if j < hkv else wq_hbm.at[j - hkv]
        return pltpu.make_async_copy(src, wst.at[j % 2], wsem.at[j % 2])

    def wo_copy(h):
        sl = lax.rem(h, 2)
        return pltpu.make_async_copy(wo_hbm.at[lay, pl.ds(pl.multiple_of(h * 2 * dh, 2 * dh), 2 * dh)], wo.at[sl], wosem.at[sl])

    load_x = pltpu.make_async_copy(x_hbm, wo.at[0, :t], msem.at[0])
    load_x.start()
    wtile(0).start()
    wtile(1).start()
    eye[...] = _eye()
    _barrier(cp, i, partner)
    load_x.wait()
    n = wo.at[1, :t]
    _cast_rows(wo.at[0, :t], x)
    _norm(x, n, g_ref[lay], 0, t)
    for j in range(2 * hkv):
        wtile(j).wait()
        y = _dot(n[...], wst[j % 2]).astype(BF16)
        for s in range(2):
            ys = y[s * r:(s + 1) * r]
            if j < hkv:
                own = slot(s, 0, c, j)
                kvg[own, :, :dh] = ys[:, :dh]
                kvg[own, :, dh:] = _turn(eye, ys[:, dh:])
                push(s, 0, j)
            else:
                for g in range(2):
                    qt[s * hkv + j - hkv, :, g * r:(g + 1) * r] = _turn(eye, ys[:, g * dh:(g + 1) * dh])
        if j + 2 < 2 * hkv:
            wtile(j + 2).start()
    wo_copy(0).start()
    wo_copy(1).start()

    def init(j):
        acc[j] = jnp.zeros(acc.shape[1:], F32)
        ml[j, 0:1, :] = jnp.full((1, 2 * r), NEG, F32)
        ml[j, 1:2, :] = jnp.zeros((1, 2 * r), F32)

    _for(2 * hkv, init)
    keys = lax.broadcasted_iota(jnp.int32, (2 * r, 2 * r), 0)
    toks = lax.broadcasted_iota(jnp.int32, (2 * r, 2 * r), 1) % r

    def flash(qi, pair, h, off=None):
        j = (pair * hkv + h) * 2
        sc = _scores(kvg[pl.ds(j, 2), :, :dh], qt[qi])
        if off is not None:
            sc = jnp.where(keys - toks <= off, sc, NEG)
        old = ml[qi, 0:1, :]
        m = jnp.maximum(old, sc.max(axis=0, keepdims=True))
        a = jnp.exp2((old - m) * scale)
        pr = jnp.exp2((sc - m) * scale)
        ml[qi, 0:1, :] = m
        ml[qi, 1:2, :] = ml[qi, 1:2, :] * a + pr.sum(axis=0, keepdims=True)
        pb = pr.astype(BF16)
        acc[qi] = acc[qi] * a + (_dot(kvg[j, :, dh:], pb[:r]) + _dot(kvg[j + 1, :, dh:], pb[r:]))

    def step(k, h):
        for s in range(2):
            got_d2d(s, k, h)

        def job(j):
            qs = jnp.where(j < 2, 1, 0)
            pair = jnp.where(j == 1, pair_of(1, k), pair_of(0, k))
            ok = jnp.where(j == 1, z + k < nz, jnp.where(j == 2, z - k >= 0, z >= 0))
            pl.when(ok)(lambda: flash(qs * hkv + h, pair, h))

        _for(3, job)

    def finish(h):
        for s in range(2):
            qi = s * hkv + h
            _store_o(eye, o, s, r, acc[qi] * (1.0 / ml[qi, 1:2, :]))
        wo_copy(h).wait()
        _out_proj(x, 0, o, wo, lax.rem(h, 2), t)
        pl.when(h + 2 < hkv)(lambda: wo_copy(h + 2).start())

    def main(j):
        k = 1 + lax.div(j, hkv)
        h = lax.rem(j, hkv)
        for s in range(2):
            got_ici(s, k, h)
            push(s, k, h)

        @pl.when(k == 1)
        def _():
            for s in range(2):
                got_d2d(s, 0, h)
            flash(h, pair_of(0, 0), h, c * r)
            flash(hkv + h, pair_of(0, 0), h)
            flash(hkv + h, pair_of(1, 0), h, (1 - c) * r)

        jp = j - 1
        kp = 1 + lax.div(jp, hkv)
        hp = lax.rem(jp, hkv)

        @pl.when(j > 0)
        def _():
            step(kp, hp)
            pl.when(kp == nz - 1)(lambda: finish(hp))

    _for((nz - 1) * hkv, main)
    step(nz - 1, hkv - 1)
    finish(hkv - 1)
    _cast_rows(x, wo.at[0, :t])
    out = pltpu.make_async_copy(wo.at[0, :t], y_hbm, msem.at[0])
    out.start()

    def drain(j):
        k = lax.div(j, hkv)
        h = lax.rem(j, hkv)
        for s in range(2):
            pl.when(sends(s, k))(lambda s=s: ici(s, k, h).wait_send())
            pl.when(has(s, k))(lambda s=s: d2d(s, k, h).wait_send())

    _for(nz * hkv, drain)
    out.wait()


def solution(mesh):
    cp = mesh.shape['cp']

    def body(x, g, wq, wk, wv, wo):
        t, d = x.shape
        r = t // 2
        nl = g.shape[0]
        hq, dh = wq.shape[2], wq.shape[3]
        hkv = wk.shape[2]
        assert (hq, hkv, dh, r, W) == (8, 4, 256, 256, 1024)
        gf = g.astype(F32).reshape(nl, 1, d)
        wq2 = wq.reshape(nl, d * hq, dh)
        wk2, wv2 = (a.reshape(nl, d, hkv, 2, dh // 2).transpose(0, 1, 3, 2, 4).reshape(nl, d * hkv * 2, dh // 2) for a in (wk, wv))
        wo2 = wo.reshape(nl, hq * dh, d)
        hbm = pl.BlockSpec(memory_space=pl.ANY)
        vmem = pl.BlockSpec(memory_space=pltpu.VMEM)
        sems = pltpu.SemaphoreType.DMA
        shape = jax.ShapeDtypeStruct
        limit = 67043328
        tile = (hkv, d, 2 * dh)
        x1, wkv_l, wq_l = pl.pallas_call(
            functools.partial(_local_kernel, cp, nl - 1),
            out_shape=(shape((t, d), BF16), shape(tile, BF16), shape(tile, BF16)),
            in_specs=[hbm, vmem, hbm, hbm, hbm, hbm],
            out_specs=(hbm, hbm, hbm),
            scratch_shapes=[
                pltpu.VMEM((t, d), F32),
                pltpu.VMEM((t, d), BF16),
                pltpu.VMEM((2 * hkv, 2 * r, dh), BF16),
                pltpu.VMEM(tile, BF16),
                pltpu.VMEM(tile, BF16),
                pltpu.VMEM((2, 2 * dh, d), BF16),
                pltpu.VMEM((2 * hkv, r, 2 * dh), BF16),
                pltpu.VMEM((2 * 2 * hkv * 2, r, 2 * dh), BF16),
                pltpu.VMEM((2 * hkv * 2, r, 2 * dh), BF16),
                pltpu.VMEM((SLOTS, d * hq // CHUNKS, dh), BF16),
                pltpu.VMEM((t, 2 * dh), BF16),
                pltpu.VMEM((256, 256), BF16),
                pltpu.VMEM((256, 256), BF16),
                sems((3,)), sems((2 * SLOTS,)), sems((2,)), sems((6 * 2 * hkv,)), sems((hkv,)), sems((2 * 2 * 4 * hkv,)),
            ],
            compiler_params=pltpu.CompilerParams(collective_id=0, has_side_effects=True, vmem_limit_bytes=limit),
            name='local_layers',
        )(x, gf, wq2, wk2, wv2, wo2)
        nz = cp // 2
        return pl.pallas_call(
            functools.partial(_global_kernel, cp, nl - 1),
            out_shape=shape((t, d), BF16),
            in_specs=[hbm, vmem, hbm, hbm, hbm],
            out_specs=hbm,
            scratch_shapes=[
                pltpu.VMEM((t, d), F32),
                pltpu.VMEM((2 * hkv, dh, 2 * r), BF16),
                pltpu.VMEM((2 * cp * hkv, r, 2 * dh), BF16),
                pltpu.VMEM((2 * hkv, dh, 2 * r), F32),
                pltpu.VMEM((2 * hkv, 8, 2 * r), F32),
                pltpu.VMEM((2, d, 2 * dh), BF16),
                pltpu.VMEM((2, 2 * dh, d), BF16),
                pltpu.VMEM((t, 2 * dh), BF16),
                pltpu.VMEM((256, 256), BF16),
                sems((1,)), sems((2,)), sems((2,)),
                sems((2 * nz * hkv,)), sems((2 * nz * hkv,)), sems((2 * nz * hkv,)), sems((2 * nz * hkv,)),
            ],
            compiler_params=pltpu.CompilerParams(collective_id=1, has_side_effects=True, vmem_limit_bytes=limit),
            name='global_layer',
        )(x1, gf, wkv_l, wq_l, wo2)

    spec = P(('dp', 'cp'), None)
    return jax.shard_map(body, mesh=mesh, in_specs=(spec, P(), P(), P(), P(), P()), out_specs=spec, check_vma=False)
```

```python
import functools
import math

import jax
import jax.numpy as jnp
from jax import lax
from jax.experimental import pallas as pl
from jax.experimental.pallas import tpu as pltpu
from jax.sharding import PartitionSpec as P

W = 1024
EPS = 1e-6
F32 = jnp.float32
BF16 = jnp.bfloat16
MESH = pl.DeviceIdType.MESH
STAGES = 4
NEG = float('-inf')

NEAR, FAR, OWN, WKV = 0, 32, 48, 56


def _dot(a, b):
    return jnp.dot(a, b, preferred_element_type=F32)


def _dot_nt(a, b):
    return lax.dot_general(a, b, (((1,), (1,)), ((), ())), preferred_element_type=F32)


def _for(n, body):
    lax.fori_loop(0, n, lambda j, c: (body(j), c)[1], 0)


def _pick(j, *vals):
    out = vals[-1]
    for k in range(len(vals) - 2, -1, -1):
        out = jnp.where(j == k, vals[k], out)
    return out


def _remote(src, dst, ssem, rsem, dev):
    return pltpu.make_async_remote_copy(src_ref=src, dst_ref=dst, send_sem=ssem, recv_sem=rsem,
                                        device_id={'cp': dev}, device_id_type=MESH)


def _blocks(lo, n, body):
    rows = 64

    def blk(j):
        body(pl.ds(pl.multiple_of(lo + j * rows, rows), rows))

    _for(n // rows, blk)


def _kernel(cp, x_hbm, g_ref, wq_hbm, wk_hbm, wv_hbm, wo_hbm, y_hbm,
            x, n, q, pool, wo, stage, o, acc, ml, gs, pq, pkv, eye,
            msem, ssem, wosem, wsend, wrecv, send, extra, recv, isend, irecv, dsend, drecv, freed, ready, wrap):
    t, d = x.shape
    r = t // 2
    nl = g_ref.shape[0]
    nloc = nl - 1
    hkv, dh = q.shape[0] // 2, q.shape[2] // 2
    nd = d // 256
    half = nd // 2
    wqb = WKV + nd * hkv
    nz = cp // 2
    i = lax.axis_index('cp')
    c = lax.rem(i, 2)
    z = lax.div(i, 2)
    partner = i + 1 - 2 * c
    up, down = lax.rem(i + 2, cp), lax.rem(i + cp - 2, cp)
    last = z == nz - 1
    scale = dh ** -0.5 * math.log2(math.e)
    h3 = hkv - 1

    lead, follow = c, 1 - c

    def dev(s):
        return jnp.where(s == 0, up, down)

    def nxt(s):
        return jnp.where(s == 0, z + 1 < nz, z > 0)

    def need(s, k):
        return (s == 1) | (z >= k)

    def sl(par, s, p, h):
        return NEAR + ((par * 2 + s) * hkv + h) * 2 + p if p < 2 else FAR + (s * hkv + h) * 2 + p - 2

    def own(s, h):
        return OWN + s * hkv + h

    def rsem(par, s, p, h):
        return recv.at[((par * 2 + s) * 4 + p) * hkv + h]

    def copy(kind, s, h, par):
        src = own(s, h) if kind in (0, 2) else sl(par, s, 3 if kind == 5 else 1, h)
        p = (1, 3, 0, 0, 2, 2)[kind]
        to = dev(s) if kind < 2 else partner
        return _remote(pool.at[src], pool.at[sl(par, s, p, h)], send.at[(kind * 2 + s) * hkv + h], rsem(par, s, p, h), to)

    def cond(kind, s):
        return (nxt(s), nxt(s) & need(s, 1), z >= 0, need(s, 1), need(s, 1), need(s, 2))[kind]

    def start(kind, s, h, par):
        pl.when(cond(kind, s))(lambda: copy(kind, s, h, par).start())

    def edge_copy(h, par):
        return _remote(pool.at[own(0, h)], pool.at[sl(par, 1, 1, h)], extra.at[h], rsem(par, 1, 1, h), partner)

    def arrived(s, p, h, par, when):
        ref = pool.at[sl(par, s, p, h)]
        pl.when(when)(lambda: pltpu.make_async_copy(ref, ref, rsem(par, s, p, h)).wait())

    def raw(kv, l, j):
        rows = pl.ds(pl.multiple_of((c * half + j) * 2048, 2048), 2048)
        slot = lax.rem(j, STAGES)
        if kv:
            return (pltpu.make_async_copy(wk_hbm.at[l, rows], stage.at[slot, :, pl.ds(0, 128)], ssem.at[slot]),
                    pltpu.make_async_copy(wv_hbm.at[l, rows], stage.at[slot, :, pl.ds(128, 128)], ssem.at[STAGES + slot]))
        return (pltpu.make_async_copy(wq_hbm.at[l, rows], stage.at[slot], ssem.at[slot]),)

    def prefetch(kv, l):
        for j in range(min(STAGES, half)):
            for cpy in raw(kv, l, j):
                cpy.start()

    def wslot(kv, core, j):
        return (WKV if kv else wqb) + (core * half + j) * hkv

    def share(kv, core, j):
        ref = pool.at[pl.ds(wslot(kv, core, j), hkv)]
        k = j if kv else half + j
        return _remote(ref, ref, wsend.at[k], wrecv.at[k], partner)

    def shared(kv):
        def one(j):
            ref = pool.at[pl.ds(wslot(kv, 1 - c, j), hkv)]
            pltpu.make_async_copy(ref, ref, wrecv.at[j if kv else half + j]).wait()
            share(kv, c, j).wait_send()

        _for(half, one)

    def relayout(kv, l, wait):
        def chunk(j):
            for cpy in raw(kv, l, j):
                cpy.wait()
            slot = lax.rem(j, STAGES)
            base = wslot(kv, c, j)
            perm = pkv[...] if kv else pq[...]
            for b in range(8):
                out = _dot(perm, stage[slot, b * 256:(b + 1) * 256, :]).astype(BF16)
                rows = slice(b * 32, (b + 1) * 32)
                for a in range(8):
                    part = out[a * 32:(a + 1) * 32]
                    if kv:
                        lane = (a % 2) * 128
                        pool[base + a // 2, rows, lane:lane + 128] = part[:, :128]
                        pool[base + a // 2, rows, dh + lane:dh + lane + 128] = part[:, 128:]
                    else:
                        pool[base + a // 2, rows, (a % 2) * dh:(a % 2 + 1) * dh] = part

            @pl.when(j + STAGES < half)
            def _():
                for cpy in raw(kv, l, j + STAGES):
                    cpy.start()

            @pl.when(j > 0)
            def _():
                share(kv, c, j - 1).start()

        if wait:
            pl.semaphore_wait(freed.at[0 if kv else 1], 1)
        _for(half, chunk)
        share(kv, c, half - 1).start()

    def release(kv):
        pl.semaphore_signal(freed.at[0 if kv else 1], inc=1, device_id={'cp': partner}, device_id_type=MESH)

    def weights(kv, h):
        base = WKV if kv else wqb
        return jnp.concatenate([pool[base + j * hkv + h] for j in range(nd)], axis=0)

    def wo_copy(l, h):
        slot = lax.rem(h, 2)
        return pltpu.make_async_copy(wo_hbm.at[l, pl.ds(pl.multiple_of(h * 2 * dh, 2 * dh), 2 * dh)], wo.at[slot], wosem.at[slot])

    def rows_of(s):
        return pl.ds(pl.multiple_of(s * r, r), r)

    def norm(s, l):
        g = gs[pl.ds(l, 1), :]

        def blk(rows):
            v = x[rows, :].astype(BF16).astype(F32)
            x[rows, :] = v
            m = lax.rsqrt(jnp.mean(v * v, axis=-1, keepdims=True) + EPS)
            n[rows, :] = (v * m * g).astype(BF16)

        _blocks(s * r, r, blk)

    def out_proj(s, slot):
        rows = rows_of(s)
        nb = min(512, d)
        for j in range(d // nb):
            cols = slice(j * nb, (j + 1) * nb)
            x[rows, cols] += _dot(o[rows, :], wo[slot, :, cols])

    def turn(a):
        return _dot_nt(eye[...], a).astype(BF16)

    load_x = pltpu.make_async_copy(x_hbm, n, msem.at[0])
    prefetch(True, 0)
    load_x.start()

    @pl.when(z < 2)
    def _():
        def clear(j):
            pool[NEAR + lax.div(j, 2 * hkv) * 4 * hkv + lax.rem(j, 2 * hkv)] = jnp.zeros(pool.shape[1:], BF16)

        def clear_far(j):
            pool[FAR + j] = jnp.zeros(pool.shape[1:], BF16)

        _for(4 * hkv, clear)
        _for(2 * hkv, clear_far)

    ro = lax.broadcasted_iota(jnp.int32, (256, 256), 0)
    co = lax.broadcasted_iota(jnp.int32, (256, 256), 1)
    pq[...] = jnp.where(co == (ro % 32) * 8 + ro // 32, 1.0, 0.0).astype(BF16)
    pkv[...] = jnp.where(co == (ro % 32) * 8 + ((ro // 32) % 2) * 4 + ro // 64, 1.0, 0.0).astype(BF16)
    eye[...] = jnp.where(ro == co, 1.0, 0.0).astype(BF16)
    for l in range(nl):
        gs[l:l + 1, :] = g_ref[l:l + 1, :].astype(F32)

    bar = pltpu.get_barrier_semaphore()
    for nb in (up, down, partner):
        pl.semaphore_signal(bar, inc=1, device_id={'cp': nb}, device_id_type=MESH)
    pl.semaphore_wait(bar, 3)

    rows2 = lax.broadcasted_iota(jnp.int32, (2 * r, r), 0) % r
    cols2 = lax.broadcasted_iota(jnp.int32, (2 * r, r), 1)

    def put_o(s, out0, out1):
        rows = rows_of(s)
        o[rows, :dh] = out0
        o[rows, dh:] = out1

    def attend(s, h, par):
        qi = s * hkv + h
        qv = jnp.concatenate([q[qi, :, :dh], q[qi, :, dh:]], axis=0)
        a = [own(s, h)] + [sl(par, s, p, h) for p in range(4)]
        sn = _dot_nt(qv, pool[pl.ds(a[1], 2), :, :dh].reshape(2 * r, dh))
        sf = _dot_nt(qv, pool[pl.ds(a[3], 2), :, :dh].reshape(2 * r, dh))
        sc = [jnp.where(cols2 <= rows2, _dot_nt(qv, pool[a[0], :, :dh]), NEG), sn[:, :r], sn[:, r:],
              sf[:, :r], jnp.where(cols2 > rows2, sf[:, r:], NEG)]
        for b in range(1, 5):
            sc[b] = sc[b] + jnp.where((s == 1) | (i >= b), 0.0, NEG).astype(F32)
        m = functools.reduce(jnp.maximum, sc).max(axis=1, keepdims=True)
        pr = [jnp.exp2((v - m) * scale) for v in sc]
        den = functools.reduce(jnp.add, pr).sum(axis=1, keepdims=True)
        num = functools.reduce(jnp.add, [_dot(v.astype(BF16), pool[b, :, dh:]) for v, b in zip(pr, a)])
        out = (num / den).astype(BF16)
        put_o(s, out[:r], out[r:])

    def local_send(s, is_lead, h, par):
        start(0, s, h, par)
        if is_lead:
            start(2, s, h, par)
        pl.when(last & (s == 0))(lambda: edge_copy(h, par).start())

    def drain(s, is_lead, h, par):
        for kind in (0, 1, 2, 4) if is_lead else (0, 1, 3, 5):
            pl.when(cond(kind, s))(lambda k=kind: copy(k, s, h, par).wait_send())
        pl.when(last & (s == 0))(lambda: edge_copy(h, par).wait_send())

    def mine(s, k, h):
        return _pick(k, own(s, h), sl(1, s, 1, h), sl(1, s, 3, h), WKV + ((k - 3) * 2 + s) * 2 * hkv + h * 2)

    def theirs(s, k, h):
        return _pick(k, sl(1, s, 0, h), sl(1, s, 2, h), sl(0, s, 0, h), WKV + ((k - 3) * 2 + s) * 2 * hkv + h * 2 + 1)

    def has(s, k):
        return jnp.where(s == 0, k < nz, z + k < nz)

    def sends(s, k):
        return jnp.where(s == 0, k < nz - 1, (z + k < nz) & (z > 0))

    def sidx(s, k, h):
        return (s * nz + k) * hkv + h

    def ici(s, k, h):
        return _remote(pool.at[mine(s, k, h)], pool.at[mine(s, k + 1, h)], isend.at[sidx(s, k, h)], irecv.at[sidx(s, k + 1, h)],
                       dev(s))

    def d2d(s, k, h):
        return _remote(pool.at[mine(s, k, h)], pool.at[theirs(s, k, h)], dsend.at[sidx(s, k, h)], drecv.at[sidx(s, k, h)], partner)

    def push(s, k, h):
        pl.when(sends(s, k))(lambda: ici(s, k, h).start())
        pl.when(has(s, k))(lambda: d2d(s, k, h).start())

    def got_ici(s, k, h):
        ref = pool.at[mine(s, k, h)]
        pl.when(has(s, k))(lambda: pltpu.make_async_copy(ref, ref, irecv.at[sidx(s, k, h)]).wait())

    def got_d2d(s, k, h):
        ref = pool.at[theirs(s, k, h)]
        pl.when(has(s, k))(lambda: pltpu.make_async_copy(ref, ref, drecv.at[sidx(s, k, h)]).wait())

    def global_kv(s, h, y):
        pool[own(s, h), :, :dh] = y[:, :dh]
        pool[own(s, h), :, dh:] = turn(y[:, dh:])
        push(s, 0, h)

    roles = ((follow, False), (lead, True))

    relayout(True, 0, False)
    load_x.wait()
    _blocks(0, t, lambda rows: x.__setitem__((rows, slice(None)), n[rows, :].astype(F32)))
    norm(follow, 0)
    prefetch(False, 0)
    shared(True)
    for s, is_lead in roles:
        if is_lead:
            norm(s, 0)
        pool[own(s, 0)] = _dot(n[rows_of(s), :], weights(True, 0)).astype(BF16)
        local_send(s, is_lead, 0, 0)
    wo_copy(0, 0).start()
    wo_copy(0, 1).start()

    def layer(l):
        par = lax.rem(l, 2)

        @pl.when((l == nloc - 1) & (z == 0))
        def _():
            pl.semaphore_signal(wrap, inc=1, device_id={'cp': down}, device_id_type=MESH)

        def kv_head(j):
            h = j + 1
            y = _dot(n[...], weights(True, h)).astype(BF16)
            for s in range(2):
                pool[own(s, h)] = y[s * r:(s + 1) * r]
            for s, is_lead in roles:
                local_send(s, is_lead, h, par)

        _for(hkv - 1, kv_head)
        release(True)

        @pl.when(l == 0)
        def _():
            relayout(False, 0, False)

        prefetch(True, l + 1)
        shared(False)

        def q_group(h):
            y = _dot(n[...], weights(False, h)).astype(BF16)
            for s in range(2):
                q[s * hkv + h] = y[s * r:(s + 1) * r]

        _for(hkv, q_group)
        release(False)

        def forward(h):
            for s, is_lead in roles:
                arrived(s, 1, h, par, need(s, 1))
            arrived(follow, 0, h, par, z >= 0)
            for s, is_lead in roles:
                for kind in (1, 4) if is_lead else (1, 3):
                    start(kind, s, h, par)

        forward(0)
        relayout(True, l + 1, True)
        prefetch(False, l + 1)
        forward(1)
        relayout(False, l + 1, True)
        forward(2)
        forward(3)
        shared(True)

        def edge(h):
            for p, core in ((2, 1), (0, 0)):
                @pl.when(last & (c == core))
                def _():
                    arrived(0, p, h, par, z >= 0)
                    pltpu.make_async_copy(pool.at[sl(par, 0, p, h)], pool.at[sl(par, 1, 3, h)], rsem(par, 1, 3, h)).start()

        def gather(s, is_lead, h):
            at_edge = last & (s == 0)
            arrived(s, 3, h, par, need(s, 2))
            if is_lead:
                arrived(s, 0, h, par, need(s, 1) & ~at_edge)
                arrived(s, 2, h, par, need(s, 2))
            else:
                start(5, s, h, par)
                arrived(s, 2, h, par, need(s, 1) & ~at_edge)

        def next_wo(h):
            wrap = lax.div(h + 2, hkv)
            wo_copy(l + wrap, h + 2 - hkv * wrap).start()

        def head(h):
            edge(h)
            for s, is_lead in roles:
                gather(s, is_lead, h)
                attend(s, h, par)
                if not is_lead:
                    wo_copy(l, h).wait()
                out_proj(s, lax.rem(h, 2))
            next_wo(h)

        _for(hkv - 1, head)
        wo_copy(l, h3).wait()
        edge(h3)
        for s, is_lead in roles:
            gather(s, is_lead, h3)
            attend(s, h3, par)
            out_proj(s, h3 % 2)
            if not is_lead:
                _for(hkv - 1, lambda h: [drain(a, b, h, par) for a, b in roles])
            drain(s, is_lead, h3, par)
            norm(s, l + 1)
            y = _dot(n[rows_of(s), :], weights(True, 0)).astype(BF16)

            @pl.when(l < nloc - 1)
            def _():
                pool[own(s, 0)] = y
                local_send(s, is_lead, 0, 1 - par)

            @pl.when(l == nloc - 1)
            def _():
                if not is_lead:
                    pl.when(last)(lambda: pl.semaphore_wait(wrap, 1))
                global_kv(s, 0, y)
        next_wo(h3)

    _for(nloc, layer)

    def kv_head(j):
        h = j + 1
        y = _dot(n[...], weights(True, h)).astype(BF16)
        for s in range(2):
            global_kv(s, h, y[s * r:(s + 1) * r])

    _for(hkv - 1, kv_head)
    shared(False)

    def q_group(h):
        y = _dot(n[...], weights(False, h)).astype(BF16)
        for s in range(2):
            for g in range(2):
                q[s * hkv + h, :, g * r:(g + 1) * r] = turn(y[s * r:(s + 1) * r, g * dh:(g + 1) * dh])

    _for(hkv, q_group)
    for nb in (up, down, partner):
        pl.semaphore_signal(ready, inc=1, device_id={'cp': nb}, device_id_type=MESH)

    def init(j):
        acc[j] = jnp.zeros(acc.shape[1:], F32)
        ml[j, 0:1, :] = jnp.full((1, 2 * r), NEG, F32)
        ml[j, 1:2, :] = jnp.zeros((1, 2 * r), F32)

    _for(2 * hkv, init)
    pl.semaphore_wait(ready, 3)
    keys = lax.broadcasted_iota(jnp.int32, (r, 2 * r), 0)
    toks = lax.broadcasted_iota(jnp.int32, (r, 2 * r), 1) % r

    def flash(qi, a, b, bias=None):
        qt = q[qi]
        sc = _dot(jnp.concatenate([pool[a, :, :dh], pool[b, :, :dh]], axis=0), qt)
        if bias is not None:
            sc = jnp.concatenate([jnp.where(keys <= toks, sc[:r], NEG), sc[r:] + bias], axis=0)
        old = ml[qi, 0:1, :]
        m = jnp.maximum(old, sc.max(axis=0, keepdims=True))
        f = jnp.exp2((old - m) * scale)
        pr = jnp.exp2((sc - m) * scale)
        ml[qi, 0:1, :] = m
        ml[qi, 1:2, :] = ml[qi, 1:2, :] * f + pr.sum(axis=0, keepdims=True)
        pb = pr.astype(BF16)
        acc[qi] = acc[qi] * f + (_dot(pool[a, :, dh:], pb[:r]) + _dot(pool[b, :, dh:], pb[r:]))

    def step(k, h):
        def job(j):
            qs = jnp.where(j < 2, 1, 0)
            ks = jnp.where(j == 1, 1, 0)
            ok = _pick(j, z >= 0, z + k < nz, z - k >= 0)
            pl.when(ok)(lambda: flash(qs * hkv + h, mine(ks, k, h), theirs(ks, k, h)))

        _for(3, job)

    def first(h):
        bias = [jnp.where(c == a, 0.0, NEG).astype(F32) for a in (1, 0)]
        flash(h, mine(0, 0, h), theirs(0, 0, h), bias[0])
        flash(hkv + h, mine(0, 0, h), theirs(0, 0, h))
        flash(hkv + h, mine(1, 0, h), theirs(1, 0, h), bias[1])

    def finish(h):
        for s in range(2):
            qi = s * hkv + h
            ob = (acc[qi] * (1.0 / ml[qi, 1:2, :])).astype(BF16)
            put_o(s, turn(ob[:, :r]), turn(ob[:, r:]))
        wo_copy(nloc, h).wait()
        for s in range(2):
            out_proj(s, lax.rem(h, 2))
        pl.when(h + 2 < hkv)(lambda: wo_copy(nloc, h + 2).start())

    def unit(u):
        k = lax.div(u, hkv)
        h = lax.rem(u, hkv)
        for s in range(2):
            got_d2d(s, k, h)
        pl.when(k == 0)(lambda: first(h))
        pl.when(k > 0)(lambda: step(k, h))
        pl.when(k == nz - 1)(lambda: finish(h))
        v = jnp.where(k == 0, u + hkv, u + 1)

        @pl.when((k == 0) | ((u >= 2 * hkv - 1) & (v < nz * hkv)))
        def _():
            kv, hv = lax.div(v, hkv), lax.rem(v, hkv)
            for s in range(2):
                got_ici(s, kv, hv)
            for s in range(2):
                push(s, kv, hv)

    _for(nz * hkv, unit)
    _blocks(0, t, lambda rows: n.__setitem__((rows, slice(None)), x[rows, :].astype(BF16)))
    out = pltpu.make_async_copy(n, y_hbm, msem.at[0])
    out.start()

    def drain_all(j):
        k = lax.div(j, hkv)
        h = lax.rem(j, hkv)
        for s in range(2):
            pl.when(sends(s, k))(lambda s=s: ici(s, k, h).wait_send())
            pl.when(has(s, k))(lambda s=s: d2d(s, k, h).wait_send())

    _for(nz * hkv, drain_all)
    out.wait()


def solution(mesh):
    cp = mesh.shape['cp']

    def body(x, g, wq, wk, wv, wo):
        t, d = x.shape
        r = t // 2
        nl = g.shape[0]
        hq, dh = wq.shape[2], wq.shape[3]
        hkv = wk.shape[2]
        nz = cp // 2
        assert (hq, hkv, dh, r, W) == (8, 4, 256, 256, 1024)
        wq2 = wq.reshape(nl, d * hq, dh)
        wk2, wv2 = (a.reshape(nl, d, hkv, 2, dh // 2).transpose(0, 1, 3, 2, 4).reshape(nl, d * hkv * 2, dh // 2) for a in (wk, wv))
        wo2 = wo.reshape(nl, hq * dh, d)
        hbm = pl.BlockSpec(memory_space=pl.ANY)
        sems = pltpu.SemaphoreType.DMA
        slots = WKV + 2 * (d // 256) * hkv
        assert slots >= WKV + (nz - 3) * 4 * hkv
        return pl.pallas_call(
            functools.partial(_kernel, cp),
            out_shape=jax.ShapeDtypeStruct((t, d), BF16),
            in_specs=[hbm, pl.BlockSpec(memory_space=pltpu.VMEM), hbm, hbm, hbm, hbm],
            out_specs=hbm,
            scratch_shapes=[
                pltpu.VMEM((t, d), F32),
                pltpu.VMEM((t, d), BF16),
                pltpu.VMEM((2 * hkv, r, 2 * dh), BF16),
                pltpu.VMEM((slots, r, 2 * dh), BF16),
                pltpu.VMEM((2, 2 * dh, d), BF16),
                pltpu.VMEM((STAGES, 2048, 256), BF16),
                pltpu.VMEM((t, 2 * dh), BF16),
                pltpu.VMEM((2 * hkv, dh, 2 * r), F32),
                pltpu.VMEM((2 * hkv, 8, 2 * r), F32),
                pltpu.VMEM((8, d), F32),
                pltpu.VMEM((256, 256), BF16),
                pltpu.VMEM((256, 256), BF16),
                pltpu.VMEM((256, 256), BF16),
                sems((1,)), sems((2 * STAGES,)), sems((2,)), sems((d // 256,)), sems((d // 256,)),
                sems((6 * 2 * hkv,)), sems((hkv,)), sems((2 * 2 * 4 * hkv,)),
                sems((2 * nz * hkv,)), sems((2 * nz * hkv,)), sems((2 * nz * hkv,)), sems((2 * nz * hkv,)),
                pltpu.SemaphoreType.REGULAR((2,)), pltpu.SemaphoreType.REGULAR, pltpu.SemaphoreType.REGULAR,
            ],
            compiler_params=pltpu.CompilerParams(collective_id=0, has_side_effects=True, vmem_limit_bytes=67043328),
            name='layers',
        )(x, g, wq2, wk2, wv2, wo2)

    spec = P(('dp', 'cp'), None)
    return jax.shard_map(body, mesh=mesh, in_specs=(spec, P(), P(), P(), P(), P()), out_specs=spec, check_vma=False)
```

```python
import functools
import math

import jax
import jax.numpy as jnp
from jax import lax
from jax.experimental import pallas as pl
from jax.experimental.pallas import tpu as pltpu
from jax.sharding import PartitionSpec as P

W = 1024
EPS = 1e-6
F32 = jnp.float32
BF16 = jnp.bfloat16
MESH = pl.DeviceIdType.MESH
STAGES = 3
STREAMS = (0, 1)
KV, Q, LEAD, FOLLOW, NO = True, False, True, False, False
TILE, LANES, ROWS = 256, 128, 2048
NEG = float('-inf')

NEAR, FAR, OWN, WKV = 0, 32, 48, 56


def _dot(a, b):
    return jnp.dot(a, b, preferred_element_type=F32)


def _dot_nt(a, b):
    return lax.dot_general(a, b, (((1,), (1,)), ((), ())), preferred_element_type=F32)


def _for(n, body):
    lax.fori_loop(0, n, lambda j, c: (body(j), c)[1], 0)


def _pick(j, *vals):
    out = vals[-1]
    for k in range(len(vals) - 2, -1, -1):
        out = jnp.where(j == k, vals[k], out)
    return out


def _remote(src, dst, ssem, rsem, dev):
    return pltpu.make_async_remote_copy(src_ref=src, dst_ref=dst, send_sem=ssem, recv_sem=rsem,
                                        device_id={'cp': dev}, device_id_type=MESH)


def _blocks(lo, n, body):
    rows = 64

    def blk(j):
        body(pl.ds(pl.multiple_of(lo + j * rows, rows), rows))

    _for(n // rows, blk)


def _kernel(cp, x_hbm, g_ref, wq_hbm, wk_hbm, wv_hbm, wo_hbm, y_hbm,
            x, n, q, pool, wo, stage, o, acc, ml, mask, gs, pq, pkv, eye,
            msem, ssem, wosem, wsend, wrecv, send, extra, recv, isend, irecv, dsend, drecv, freed, ready, wrap, credit):
    t, d = x.shape
    r = t // 2
    nl = g_ref.shape[0]
    nloc = nl - 1
    hkv, dh = q.shape[0] // 2, q.shape[2] // 2
    nd = d // 256
    half = nd // 2
    wqb = WKV + nd * hkv
    nz = cp // 2
    i = lax.axis_index('cp')
    c = lax.rem(i, 2)
    z = lax.div(i, 2)
    partner = i + 1 - 2 * c
    up, down = lax.rem(i + 2, cp), lax.rem(i + cp - 2, cp)
    last = z == nz - 1
    scale = dh ** -0.5 * math.log2(math.e)
    h3 = hkv - 1
    hh = 2 * hkv

    lead, follow = c, 1 - c

    def dev(s):
        return jnp.where(s == 0, up, down)

    def nxt(s):
        return jnp.where(s == 0, z + 1 < nz, z > 0)

    def need(s, k):
        return (s == 1) | (z >= k)

    def sl(par, s, p, h):
        return NEAR + ((par * 2 + s) * hkv + h) * 2 + p if p < 2 else FAR + (s * hkv + h) * 2 + p - 2

    def own(s, h):
        return OWN + s * hkv + h

    def rsem(par, s, p, h):
        return recv.at[((par * 2 + s) * 4 + p) * hkv + h]

    def copy(kind, s, h, par):
        src = own(s, h) if kind in (0, 2) else sl(par, s, 3 if kind == 5 else 1, h)
        p = (1, 3, 0, 0, 2, 2)[kind]
        to = dev(s) if kind < 2 else partner
        return _remote(pool.at[src], pool.at[sl(par, s, p, h)], send.at[(kind * 2 + s) * hkv + h], rsem(par, s, p, h), to)

    def cond(kind, s):
        return (nxt(s), nxt(s) & need(s, 1), z >= 0, need(s, 1), need(s, 1), need(s, 2))[kind]

    def start(kind, s, h, par):
        pl.when(cond(kind, s))(lambda: copy(kind, s, h, par).start())

    def edge_copy(h, par):
        return _remote(pool.at[own(0, h)], pool.at[sl(par, 1, 1, h)], extra.at[h], rsem(par, 1, 1, h), partner)

    def arrived(s, p, h, par, when):
        ref = pool.at[sl(par, s, p, h)]
        pl.when(when)(lambda: pltpu.make_async_copy(ref, ref, rsem(par, s, p, h)).wait())

    def raw(kv, l, j, base):
        rows = pl.ds(pl.multiple_of((base + j) * ROWS, ROWS), ROWS)
        slot = lax.rem(j, STAGES)
        if kv:
            return (pltpu.make_async_copy(wk_hbm.at[l, rows], stage.at[slot, :, pl.ds(0, LANES)], ssem.at[slot]),
                    pltpu.make_async_copy(wv_hbm.at[l, rows], stage.at[slot, :, pl.ds(LANES, LANES)], ssem.at[STAGES + slot]))
        return (pltpu.make_async_copy(wq_hbm.at[l, rows], stage.at[slot], ssem.at[slot]),)

    def prefetch(kv, l, base=c * half, count=half):
        for j in range(min(STAGES, count)):
            for cpy in raw(kv, l, j, base):
                cpy.start()

    def wslot(kv, core, j):
        return (WKV if kv else wqb) + (core * half + j) * hkv

    def share(kv, core, j):
        ref = pool.at[pl.ds(wslot(kv, core, j), hkv)]
        k = j if kv else half + j
        return _remote(ref, ref, wsend.at[k], wrecv.at[k], partner)

    def shared(kv):
        def one(j):
            ref = pool.at[pl.ds(wslot(kv, 1 - c, j), hkv)]
            pltpu.make_async_copy(ref, ref, wrecv.at[j if kv else half + j]).wait()
            share(kv, c, j).wait_send()

        _for(half, one)

    def relayout(kv, l, sharing, first=c * half, count=half):
        def chunk(j):
            for cpy in raw(kv, l, j, first):
                cpy.wait()
            slot = lax.rem(j, STAGES)
            base = (WKV if kv else wqb) + (first + j) * hkv
            perm = pkv[...] if kv else pq[...]
            for b in range(8):
                out = _dot(perm, stage[slot, b * 256:(b + 1) * 256, :]).astype(BF16)
                rows = slice(b * 32, (b + 1) * 32)
                for a in range(8):
                    part = out[a * 32:(a + 1) * 32]
                    if kv:
                        lane = (a % 2) * LANES
                        pool[base + a // 2, rows, lane:lane + LANES] = part[:, :LANES]
                        pool[base + a // 2, rows, dh + lane:dh + lane + LANES] = part[:, LANES:]
                    else:
                        pool[base + a // 2, rows, (a % 2) * dh:(a % 2 + 1) * dh] = part

            @pl.when(j + STAGES < count)
            def _():
                for cpy in raw(kv, l, j + STAGES, first):
                    cpy.start()

            if sharing:
                pl.when(j > 0)(lambda: share(kv, c, j - 1).start())

        _for(count, chunk)
        if sharing:
            share(kv, c, half - 1).start()

    def share_all(kv):
        _for(half, lambda j: share(kv, c, j).start())

    def release(kv):
        pl.semaphore_signal(freed.at[0 if kv else 1], inc=1, device_id={'cp': partner}, device_id_type=MESH)

    def weights(kv, h):
        base = WKV if kv else wqb
        return jnp.concatenate([pool[base + j * hkv + h] for j in range(nd)], axis=0)

    def wo_copy(l, e):
        slot = lax.rem(e, 2)
        rows = pl.ds(pl.multiple_of(lax.rem(e, hkv) * 2 * dh, 2 * dh), 2 * dh)
        return pltpu.make_async_copy(wo_hbm.at[l, rows], wo.at[slot], wosem.at[slot])

    def rows_of(s):
        return pl.ds(pl.multiple_of(s * r, r), r)

    def norm(s, l):
        g = gs[pl.ds(l, 1), :]

        def blk(rows):
            v = x[rows, :].astype(BF16).astype(F32)
            x[rows, :] = v
            m = lax.rsqrt(jnp.mean(v * v, axis=-1, keepdims=True) + EPS)
            n[rows, :] = (v * m * g).astype(BF16)

        _blocks(s * r, r, blk)

    def out_tiles(s, h, slot, nb):
        rows = rows_of(s)

        def tile(j):
            cols = slice(j * nb, (j + 1) * nb)
            x[rows, cols] += _dot(o[lax.rem(h, 2), rows, :], wo[slot, :, cols])

        return [functools.partial(tile, j) for j in range(d // nb)]

    def out_proj(s, h, slot):
        for tile in out_tiles(s, h, slot, min(512, d)):
            tile()

    def turn(a):
        return _dot_nt(eye[...], a).astype(BF16)

    bar = pltpu.get_barrier_semaphore()
    for nb in (up, down, partner):
        pl.semaphore_signal(bar, inc=1, device_id={'cp': nb}, device_id_type=MESH)
    load_x = pltpu.make_async_copy(x_hbm, n, msem.at[0])
    load_x.start()
    prefetch(KV, 0, 0, nd)

    ro = lax.broadcasted_iota(jnp.int32, (TILE, TILE), 0)
    co = lax.broadcasted_iota(jnp.int32, (TILE, TILE), 1)
    pq[...] = jnp.where(co == (ro % 32) * 8 + ro // 32, 1.0, 0.0).astype(BF16)
    pkv[...] = jnp.where(co == (ro % 32) * 8 + ((ro // 32) % 2) * 4 + ro // 64, 1.0, 0.0).astype(BF16)
    eye[...] = jnp.where(ro == co, 1.0, 0.0).astype(BF16)
    mask[0] = jnp.where(co <= ro, 0.0, NEG).astype(F32)
    mask[1] = jnp.where(co > ro, 0.0, NEG).astype(F32)
    for l in range(nl):
        gs[l:l + 1, :] = g_ref[l:l + 1, :].astype(F32)


    def put_o(s, h, out0, out1):
        rows = rows_of(s)
        o[lax.rem(h, 2), rows, :dh] = out0
        o[lax.rem(h, 2), rows, dh:] = out1

    def attend(s, h, par, fill):
        qi = s * hkv + h
        qv = jnp.concatenate([q[qi, :, :dh], q[qi, :, dh:]], axis=0)
        a = [own(s, h)] + [sl(par, s, p, h) for p in range(4)]
        s0 = _dot_nt(qv, pool[a[0], :, :dh])
        sn = _dot_nt(qv, pool[pl.ds(a[1], 2), :, :dh].reshape(t, dh))
        sf = _dot_nt(qv, pool[pl.ds(a[3], 2), :, :dh].reshape(t, dh))
        miss = [jnp.where((s == 1) | (i >= b), 0.0, NEG).astype(F32) for b in range(5)]
        ch = 64
        probs, inv = [], []
        fill = list(fill)
        steps = 2 * r // ch
        for k in range(steps):
            rows = slice(k * ch, (k + 1) * ch)
            lo = k * ch % r
            sc = [s0[rows] + mask[0, lo:lo + ch, :], sn[rows, :r], sn[rows, r:], sf[rows, :r],
                  sf[rows, r:] + mask[1, lo:lo + ch, :]]
            tops = [jnp.maximum(v[:, :LANES], v[:, LANES:]) for v in sc]
            tops = [tops[0]] + [v + miss[b] for b, v in enumerate(tops) if b]
            m = functools.reduce(jnp.maximum, tops).max(axis=1, keepdims=True) * scale
            pr = [jnp.exp2(v * scale - (m - miss[b])) for b, v in enumerate(sc)]
            inv.append(1.0 / functools.reduce(jnp.add, pr).sum(axis=1, keepdims=True))
            probs.append([v.astype(BF16) for v in pr])
            for _ in range(-(-len(fill) // (steps - k))):
                fill.pop(0)()
        pb = [jnp.concatenate([v[b] for v in probs], axis=0) for b in range(5)]
        num = functools.reduce(jnp.add, [_dot(v, pool[b, :, dh:]) for v, b in zip(pb, a)])
        out = (num * jnp.concatenate(inv, axis=0)).astype(BF16)
        put_o(s, h, out[:r], out[r:])

    def local_send(s, is_lead, h, par):
        start(0, s, h, par)
        if is_lead:
            start(2, s, h, par)
        pl.when(last & (s == 0))(lambda: edge_copy(h, par).start())

    def drain(s, is_lead, h, par):
        for kind in (0, 1, 2, 4) if is_lead else (0, 1, 3, 5):
            pl.when(cond(kind, s))(lambda k=kind: copy(k, s, h, par).wait_send())
        pl.when(last & (s == 0))(lambda: edge_copy(h, par).wait_send())

    def mine(s, k, h):
        return _pick(k, own(s, h), sl(1, s, 1, h), sl(1, s, 3, h), WKV + ((k - 3) * 2 + s) * hh + h * 2)

    def theirs(s, k, h):
        return _pick(k, sl(1, s, 0, h), sl(1, s, 2, h), sl(0, s, 0, h), WKV + ((k - 3) * 2 + s) * hh + h * 2 + 1)

    def has(s, k):
        return jnp.where(s == 0, k < nz, z + k < nz)

    def sends(s, k):
        return jnp.where(s == 0, k < nz - 1, (z + k < nz) & (z > 0))

    def sidx(s, k, h):
        return (s * nz + k) * hkv + h

    def ici(s, k, h):
        return _remote(pool.at[mine(s, k, h)], pool.at[mine(s, k + 1, h)], isend.at[sidx(s, k, h)], irecv.at[sidx(s, k + 1, h)],
                       dev(s))

    def d2d(s, k, h):
        return _remote(pool.at[mine(s, k, h)], pool.at[theirs(s, k, h)], dsend.at[sidx(s, k, h)], drecv.at[sidx(s, k, h)], partner)

    def push(s, k, h):
        pl.when(sends(s, k))(lambda: ici(s, k, h).start())
        pl.when(has(s, k))(lambda: d2d(s, k, h).start())

    def got_ici(s, k, h):
        ref = pool.at[mine(s, k, h)]
        pl.when(has(s, k))(lambda: pltpu.make_async_copy(ref, ref, irecv.at[sidx(s, k, h)]).wait())

    def got_d2d(s, k, h):
        ref = pool.at[theirs(s, k, h)]
        pl.when(has(s, k))(lambda: pltpu.make_async_copy(ref, ref, drecv.at[sidx(s, k, h)]).wait())

    def global_kv(s, h, y):
        pool[own(s, h), :, :dh] = y[:, :dh]
        pool[own(s, h), :, dh:] = turn(y[:, dh:])
        push(s, 0, h)

    roles = ((follow, FOLLOW), (lead, LEAD))

    def local_keys(s, is_lead, par):
        def one(h):
            pool[own(s, h)] = _dot(n[rows_of(s), :], weights(KV, h)).astype(BF16)
            local_send(s, is_lead, h, par)

        _for(hkv, one)

    def global_keys(s):
        _for(hkv, lambda h: global_kv(s, h, _dot(n[rows_of(s), :], weights(KV, h)).astype(BF16)))

    def forward(is_lead, h, l, par):
        s = lead if is_lead else follow
        arrived(s, 1, h, par, need(s, 1))
        if is_lead:
            arrived(follow, 0, h, par, z >= 0)
        pl.when((h == 0) & (l > 0) & cond(1, s))(lambda: pl.semaphore_wait(credit.at[int(is_lead)], 1))
        for kind in (1, 4) if is_lead else (1, 3):
            start(kind, s, h, par)

    def relay_early(h):
        got_ici(follow, 1, h)
        pl.when((h == 0) & sends(follow, 1))(lambda: pl.semaphore_wait(credit.at[0], 1))
        pl.when(sends(follow, 1))(lambda: ici(follow, 1, h).start())

    def give_credit(is_lead, final):
        s = lead if is_lead else follow
        giver = jnp.where(s == 0, final | (z >= 2), jnp.where(final, z + 2 < nz, z + 1 < nz))

        @pl.when(giver)
        def _():
            to = jnp.where(s == 0, down, up)
            pl.semaphore_signal(credit.at[int(is_lead)], inc=1, device_id={'cp': to}, device_id_type=MESH)

    def clear():
        def one(h):
            for p, when in enumerate(((z == 0) & (c == 0), z == 0, (z == 0) | ((z == 1) & (c == 0)), z < 2)):
                for par in range(2 if p < 2 else 1):
                    pl.when(when)(lambda p=p, par=par: pool.__setitem__(sl(par, 0, p, h), jnp.zeros(pool.shape[1:], BF16)))

        _for(hkv, one)

    with jax.named_scope('entry_x'):
        load_x.wait()
        _blocks(0, t, lambda rows: x.__setitem__((rows, slice(None)), n[rows, :].astype(F32)))
        norm(follow, 0)
    with jax.named_scope('entry_kv'):
        relayout(KV, 0, NO, 0, nd)
        prefetch(Q, 0)
        wo_copy(0, 0).start()
        wo_copy(0, 1).start()
    with jax.named_scope('entry_barrier'):
        pl.semaphore_wait(bar, 3)
    with jax.named_scope('entry_keys_f'):
        local_keys(follow, FOLLOW, 0)
    with jax.named_scope('entry_q'):
        relayout(Q, 0, True)
    with jax.named_scope('entry_keys_l'):
        norm(lead, 0)
        pl.when(z < 2)(clear)
        for h in range(h3):
            forward(FOLLOW, h, 0, 0)
        local_keys(lead, LEAD, 0)
        release(KV)

    def layer(l):
        par = lax.rem(l, 2)
        final = l == nloc - 1

        @pl.when(final & (z == 0))
        def _():
            pl.semaphore_signal(wrap, inc=1, device_id={'cp': down}, device_id_type=MESH)

        with jax.named_scope('q'):
            prefetch(KV, l + 1)
            shared(Q)

            def q_group(h):
                y = _dot(n[...], weights(Q, h)).astype(BF16)
                for s in STREAMS:
                    q[s * hkv + h] = y[s * r:(s + 1) * r]

            _for(hkv, q_group)
            release(Q)
        with jax.named_scope('forward_a'):
            forward(FOLLOW, h3, l, par)
            forward(LEAD, 0, l, par)
        with jax.named_scope('relayout_kv'):
            pl.semaphore_wait(freed.at[0], 1)
            relayout(KV, l + 1, True)
            prefetch(Q, l + 1)

        def edge(h):
            for p, core in ((2, 1), (0, 0)):
                @pl.when(last & (c == core))
                def _():
                    arrived(0, p, h, par, z >= 0)
                    pltpu.make_async_copy(pool.at[sl(par, 0, p, h)], pool.at[sl(par, 1, 3, h)], rsem(par, 1, 3, h)).start()

        def gather(s, is_lead, h):
            at_edge = last & (s == 0)
            if not is_lead:
                edge(h)
            arrived(s, 3, h, par, need(s, 2))
            if is_lead:
                arrived(s, 0, h, par, need(s, 1) & ~at_edge)
                arrived(s, 2, h, par, need(s, 2))
            else:
                start(5, s, h, par)
                arrived(s, 2, h, par, need(s, 1) & ~at_edge)

        def use(is_lead, h):
            return h + (hkv if is_lead else 0)

        def next_wo(e):
            wrapped = lax.div(e + 2, hh)
            wo_copy(l + wrapped, e + 2 - hh * wrapped).start()

        def head(s, is_lead, h, first):
            with jax.named_scope('gather'):
                gather(s, is_lead, h)
                if not first:
                    wo_copy(l, use(is_lead, h - 1)).wait()
            with jax.named_scope('attend'):
                attend(s, h, par, [] if first else out_tiles(s, h - 1, lax.rem(h - 1, 2), 256))
            if not first:
                next_wo(use(is_lead, h - 1))

        def heads(s, is_lead, after):
            head(s, is_lead, 0, True)
            after(0)

            def one(j):
                head(s, is_lead, j + 1, False)
                after(j + 1)

            _for(h3, one)

        def tail(s, is_lead):
            with jax.named_scope('out'):
                wo_copy(l, use(is_lead, h3)).wait()
                out_proj(s, h3, h3 % 2)
                next_wo(use(is_lead, h3))
            with jax.named_scope('norm'):
                norm(s, l + 1)
            with jax.named_scope('drain'):
                _for(hkv, lambda h: drain(s, is_lead, h, par))
                if is_lead:
                    pl.when(~final)(lambda: give_credit(is_lead, False))
                else:
                    give_credit(is_lead, final)
            with jax.named_scope('keys'):
                @pl.when(~final)
                def _():
                    local_keys(s, is_lead, 1 - par)

                @pl.when(final)
                def _():
                    if not is_lead:
                        pl.when(last)(lambda: pl.semaphore_wait(wrap, 1))
                    global_keys(s)

        def ahead(h):
            pl.when(~final)(lambda: forward(FOLLOW, h, l + 1, 1 - par))
            pl.when(final)(lambda: relay_early(h))

        def after_f(h):
            pl.when(h == 0)(lambda: forward(LEAD, 1, l, par))

            @pl.when(h == 1)
            def _():
                relayout(Q, l + 1, NO)
                forward(LEAD, 2, l, par)
                forward(LEAD, 3, l, par)
                shared(KV)

        def after_l(h):
            pl.when(h == 1)(lambda: ahead(0))
            pl.when(h == 2)(lambda: ahead(1))

        heads(follow, FOLLOW, after_f)
        pl.semaphore_wait(freed.at[1], 1)
        share_all(Q)
        tail(follow, FOLLOW)
        heads(lead, LEAD, after_l)
        ahead(2)
        tail(lead, LEAD)
        pl.when(~final)(lambda: release(KV))

    _for(nloc, layer)

    shared(Q)

    def q_group(h):
        y = _dot(n[...], weights(Q, h)).astype(BF16)
        for s in STREAMS:
            for g in range(2):
                q[s * hkv + h, :, g * r:(g + 1) * r] = turn(y[s * r:(s + 1) * r, g * dh:(g + 1) * dh])

    _for(hkv, q_group)
    for nb in (up, down, partner):
        pl.semaphore_signal(ready, inc=1, device_id={'cp': nb}, device_id_type=MESH)

    def init(j):
        acc[j] = jnp.zeros(acc.shape[1:], F32)
        ml[j, 0:1, :] = jnp.full((1, t), NEG, F32)
        ml[j, 1:2, :] = jnp.zeros((1, t), F32)

    _for(hh, init)
    pl.semaphore_wait(ready, 3)

    def relay(s, k, h):
        got_ici(s, k, h)
        push(s, k, h)

    relay_early(h3)
    _for(hkv, lambda h: pl.when(has(follow, 1))(lambda: d2d(follow, 1, h).start()))
    keys = lax.broadcasted_iota(jnp.int32, (r, t), 0)
    toks = lax.broadcasted_iota(jnp.int32, (r, t), 1) % r

    def flash(qi, a, b, bias=None):
        qt = q[qi]
        sc = _dot(jnp.concatenate([pool[a, :, :dh], pool[b, :, :dh]], axis=0), qt)
        if bias is not None:
            sc = jnp.concatenate([jnp.where(keys <= toks, sc[:r], NEG), sc[r:] + bias], axis=0)
        old = ml[qi, 0:1, :]
        m = jnp.maximum(old, sc.max(axis=0, keepdims=True))
        f = jnp.exp2((old - m) * scale)
        pr = jnp.exp2((sc - m) * scale)
        ml[qi, 0:1, :] = m
        ml[qi, 1:2, :] = ml[qi, 1:2, :] * f + pr.sum(axis=0, keepdims=True)
        pb = pr.astype(BF16)
        acc[qi] = acc[qi] * f + (_dot(pool[a, :, dh:], pb[:r]) + _dot(pool[b, :, dh:], pb[r:]))

    def step(k, h):
        def job(j):
            qs = jnp.where(j < 2, 1, 0)
            ks = jnp.where(j == 1, 1, 0)
            ok = _pick(j, z >= 0, z + k < nz, z - k >= 0)
            pl.when(ok)(lambda: flash(qs * hkv + h, mine(ks, k, h), theirs(ks, k, h)))

        _for(3, job)

    def first(h):
        bias = [jnp.where(c == a, 0.0, NEG).astype(F32) for a in (1, 0)]
        flash(h, mine(0, 0, h), theirs(0, 0, h), bias[0])
        flash(hkv + h, mine(0, 0, h), theirs(0, 0, h))
        flash(hkv + h, mine(1, 0, h), theirs(1, 0, h), bias[1])

    def finish_o(s, h):
        qi = s * hkv + h
        ob = (acc[qi] * (1.0 / ml[qi, 1:2, :])).astype(BF16)
        put_o(s, h, turn(ob[:, :r]), turn(ob[:, r:]))

    def finish(h):
        for s in STREAMS:
            finish_o(s, h)
        wo_copy(nloc, h).wait()
        for s in STREAMS:
            out_proj(s, h, lax.rem(h, 2))
        pl.when(h + 2 < hkv)(lambda: wo_copy(nloc, h + 2).start())

    def put(rows):
        n[rows, :] = x[rows, :].astype(BF16)
        pltpu.make_async_copy(n.at[rows], y_hbm.at[rows], msem.at[0]).start()

    def drain_unit(j):
        k, h = lax.div(j, hkv), lax.rem(j, hkv)
        for s in STREAMS:
            pl.when(sends(s, k))(lambda s=s: ici(s, k, h).wait_send())
            pl.when(has(s, k))(lambda s=s: d2d(s, k, h).wait_send())

    def ready_keys(k, h):
        with jax.named_scope('got'):
            for s in STREAMS:
                got_d2d(s, k, h)

    def unit(u):
        k = lax.div(u, hkv)
        h = lax.rem(u, hkv)
        ready_keys(k, h)
        with jax.named_scope('flash'):
            pl.when(k == 0)(lambda: first(h))
            pl.when(k > 0)(lambda: step(k, h))
        with jax.named_scope('finish'):
            pl.when(k == nz - 1)(lambda: finish(h))
            pl.when(k > 1)(lambda: drain_unit(u - hh))
        pl.when(k == 0)(lambda: relay(lead, 1, h))
        v = u + 1

        @pl.when((v >= hh) & (v < nz * hkv))
        def _():
            for s in STREAMS:
                relay(s, lax.div(v, hkv), lax.rem(v, hkv))

    units = nz * hkv
    with jax.named_scope('units'):
        _for(units - 1, unit)
    _for(hkv + 1, lambda j: drain_unit(units - hh - 1 + j))
    wo_copy(nloc, h3).wait()
    ready_keys(nz - 1, h3)
    with jax.named_scope('flash'):
        step(nz - 1, h3)
    with jax.named_scope('end'):
        for s in STREAMS:
            finish_o(s, h3)
        for s in STREAMS:
            out_proj(s, h3, h3 % 2)
            _blocks(s * r, r, put)
        _for(hkv, lambda j: drain_unit(units - hkv + j))
        pltpu.make_async_copy(n, y_hbm, msem.at[0]).wait()


def solution(mesh):
    cp = mesh.shape['cp']

    def body(x, g, wq, wk, wv, wo):
        t, d = x.shape
        r = t // 2
        nl = g.shape[0]
        hq, dh = wq.shape[2], wq.shape[3]
        hkv = wk.shape[2]
        nz = cp // 2
        assert (hq, hkv, dh, r, W) == (8, 4, 256, 256, 1024)
        wq2 = wq.reshape(nl, d * hq, dh)
        wk2, wv2 = (a.reshape(nl, d, hkv, 2, dh // 2).transpose(0, 1, 3, 2, 4).reshape(nl, d * hkv * 2, dh // 2) for a in (wk, wv))
        wo2 = wo.reshape(nl, hq * dh, d)
        hbm = pl.BlockSpec(memory_space=pl.ANY)
        sems = pltpu.SemaphoreType.DMA
        slots = WKV + 2 * (d // 256) * hkv
        assert slots >= WKV + (nz - 3) * 4 * hkv
        return pl.pallas_call(
            functools.partial(_kernel, cp),
            out_shape=jax.ShapeDtypeStruct((t, d), BF16),
            in_specs=[hbm, pl.BlockSpec(memory_space=pltpu.VMEM), hbm, hbm, hbm, hbm],
            out_specs=hbm,
            scratch_shapes=[
                pltpu.VMEM((t, d), F32),
                pltpu.VMEM((t, d), BF16),
                pltpu.VMEM((2 * hkv, r, 2 * dh), BF16),
                pltpu.VMEM((slots, r, 2 * dh), BF16),
                pltpu.VMEM((2, 2 * dh, d), BF16),
                pltpu.VMEM((STAGES, ROWS, 256), BF16),
                pltpu.VMEM((2, t, 2 * dh), BF16),
                pltpu.VMEM((2 * hkv, dh, 2 * r), F32),
                pltpu.VMEM((2 * hkv, 8, 2 * r), F32),
                pltpu.VMEM((2, r, r), F32),
                pltpu.VMEM((8, d), F32),
                pltpu.VMEM((TILE, TILE), BF16),
                pltpu.VMEM((TILE, TILE), BF16),
                pltpu.VMEM((TILE, TILE), BF16),
                sems((1,)), sems((2 * STAGES,)), sems((2,)), sems((d // 256,)), sems((d // 256,)),
                sems((6 * 2 * hkv,)), sems((hkv,)), sems((2 * 2 * 4 * hkv,)),
                sems((2 * nz * hkv,)), sems((2 * nz * hkv,)), sems((2 * nz * hkv,)), sems((2 * nz * hkv,)),
                pltpu.SemaphoreType.REGULAR((2,)), pltpu.SemaphoreType.REGULAR, pltpu.SemaphoreType.REGULAR,
                pltpu.SemaphoreType.REGULAR((2,)),
            ],
            compiler_params=pltpu.CompilerParams(collective_id=0, has_side_effects=True, vmem_limit_bytes=67043328),
            name='layers',
        )(x, g, wq2, wk2, wv2, wo2)

    spec = P(('dp', 'cp'), None)
    return jax.shard_map(body, mesh=mesh, in_specs=(spec, P(), P(), P(), P(), P()), out_specs=spec, check_vma=False)
```

```python
import functools
import math

import jax
import jax.numpy as jnp
from jax import lax
from jax.experimental import pallas as pl
from jax.experimental.pallas import tpu as pltpu
from jax.sharding import PartitionSpec as P

W = 1024
EPS = 1e-6
F32 = jnp.float32
BF16 = jnp.bfloat16
MESH = pl.DeviceIdType.MESH
STAGES = 3
STREAMS = (0, 1)
KV, Q, LEAD, FOLLOW, NO = True, False, True, False, False
TILE, LANES, ROWS = 256, 128, 2048
NEG = float('-inf')

NEAR, FAR, OWN, WKV = 0, 32, 48, 56


def _dot(a, b):
    return jnp.dot(a, b, preferred_element_type=F32)


def _dot_nt(a, b):
    return lax.dot_general(a, b, (((1,), (1,)), ((), ())), preferred_element_type=F32)


def _for(n, body):
    lax.fori_loop(0, n, lambda j, c: (body(j), c)[1], 0)


def _pick(j, *vals):
    out = vals[-1]
    for k in range(len(vals) - 2, -1, -1):
        out = jnp.where(j == k, vals[k], out)
    return out


def _remote(src, dst, ssem, rsem, dev):
    return pltpu.make_async_remote_copy(src_ref=src, dst_ref=dst, send_sem=ssem, recv_sem=rsem,
                                        device_id={'cp': dev}, device_id_type=MESH)


def _blocks(lo, n, body):
    rows = 64

    def blk(j):
        body(pl.ds(pl.multiple_of(lo + j * rows, rows), rows))

    _for(n // rows, blk)


def _kernel(cp, x_hbm, g_ref, wq_hbm, wk_hbm, wv_hbm, wo_hbm, y_hbm,
            x, n, q, pool, wo, stage, o, acc, ml, mask, gs, pq, pkv, eye,
            msem, ssem, wosem, wsend, wrecv, send, extra, recv, isend, irecv, dsend, drecv, freed, ready, wrap, credit):
    t, d = x.shape
    r = t // 2
    nl = g_ref.shape[0]
    nloc = nl - 1
    hkv, dh = q.shape[0] // 2, q.shape[2] // 2
    nd = d // 256
    half = nd // 2
    wqb = WKV + nd * hkv
    nz = cp // 2
    i = lax.axis_index('cp')
    c = lax.rem(i, 2)
    z = lax.div(i, 2)
    partner = i + 1 - 2 * c
    up, down = lax.rem(i + 2, cp), lax.rem(i + cp - 2, cp)
    last = z == nz - 1
    scale = dh ** -0.5 * math.log2(math.e)
    h3 = hkv - 1
    hh = 2 * hkv

    lead, follow = c, 1 - c

    def dev(s):
        return jnp.where(s == 0, up, down)

    def nxt(s):
        return jnp.where(s == 0, z + 1 < nz, z > 0)

    def need(s, k):
        return (s == 1) | (z >= k)

    def sl(par, s, p, h):
        return NEAR + ((par * 2 + s) * hkv + h) * 2 + p if p < 2 else FAR + (s * hkv + h) * 2 + p - 2

    def own(s, h):
        return OWN + s * hkv + h

    def rsem(par, s, p, h):
        return recv.at[((par * 2 + s) * 4 + p) * hkv + h]

    def copy(kind, s, h, par):
        src = own(s, h) if kind in (0, 2) else sl(par, s, 3 if kind == 5 else 1, h)
        p = (1, 3, 0, 0, 2, 2)[kind]
        to = dev(s) if kind < 2 else partner
        return _remote(pool.at[src], pool.at[sl(par, s, p, h)], send.at[(kind * 2 + s) * hkv + h], rsem(par, s, p, h), to)

    def cond(kind, s):
        return (nxt(s), nxt(s) & need(s, 1), z >= 0, need(s, 1), need(s, 1), need(s, 2))[kind]

    def start(kind, s, h, par):
        pl.when(cond(kind, s))(lambda: copy(kind, s, h, par).start())

    def edge_copy(h, par):
        return _remote(pool.at[own(0, h)], pool.at[sl(par, 1, 1, h)], extra.at[h], rsem(par, 1, 1, h), partner)

    def arrived(s, p, h, par, when):
        ref = pool.at[sl(par, s, p, h)]
        pl.when(when)(lambda: pltpu.make_async_copy(ref, ref, rsem(par, s, p, h)).wait())

    def raw(kv, l, j, base):
        rows = pl.ds(pl.multiple_of((base + j) * ROWS, ROWS), ROWS)
        slot = lax.rem(j, STAGES)
        if kv:
            return (pltpu.make_async_copy(wk_hbm.at[l, rows], stage.at[slot, :, pl.ds(0, LANES)], ssem.at[slot]),
                    pltpu.make_async_copy(wv_hbm.at[l, rows], stage.at[slot, :, pl.ds(LANES, LANES)], ssem.at[STAGES + slot]))
        return (pltpu.make_async_copy(wq_hbm.at[l, rows], stage.at[slot], ssem.at[slot]),)

    def prefetch(kv, l, base=c * half, count=half):
        for j in range(min(STAGES, count)):
            for cpy in raw(kv, l, j, base):
                cpy.start()

    def wslot(kv, core, j):
        return (WKV if kv else wqb) + (core * half + j) * hkv

    def share(kv, core, j):
        ref = pool.at[pl.ds(wslot(kv, core, j), hkv)]
        k = j if kv else half + j
        return _remote(ref, ref, wsend.at[k], wrecv.at[k], partner)

    def shared(kv):
        def one(j):
            ref = pool.at[pl.ds(wslot(kv, 1 - c, j), hkv)]
            pltpu.make_async_copy(ref, ref, wrecv.at[j if kv else half + j]).wait()
            share(kv, c, j).wait_send()

        _for(half, one)

    def relayout(kv, l, sharing, first=c * half, count=half):
        def chunk(j):
            for cpy in raw(kv, l, j, first):
                cpy.wait()
            slot = lax.rem(j, STAGES)
            base = (WKV if kv else wqb) + (first + j) * hkv
            perm = pkv[...] if kv else pq[...]
            for b in range(8):
                out = _dot(perm, stage[slot, b * 256:(b + 1) * 256, :]).astype(BF16)
                rows = slice(b * 32, (b + 1) * 32)
                for a in range(8):
                    part = out[a * 32:(a + 1) * 32]
                    if kv:
                        lane = (a % 2) * LANES
                        pool[base + a // 2, rows, lane:lane + LANES] = part[:, :LANES]
                        pool[base + a // 2, rows, dh + lane:dh + lane + LANES] = part[:, LANES:]
                    else:
                        pool[base + a // 2, rows, (a % 2) * dh:(a % 2 + 1) * dh] = part

            @pl.when(j + STAGES < count)
            def _():
                for cpy in raw(kv, l, j + STAGES, first):
                    cpy.start()

            if sharing:
                pl.when(j > 0)(lambda: share(kv, c, j - 1).start())

        _for(count, chunk)
        if sharing:
            share(kv, c, half - 1).start()

    def share_all(kv):
        _for(half, lambda j: share(kv, c, j).start())

    def release(kv):
        pl.semaphore_signal(freed.at[0 if kv else 1], inc=1, device_id={'cp': partner}, device_id_type=MESH)

    def weights(kv, h):
        base = WKV if kv else wqb
        return jnp.concatenate([pool[base + j * hkv + h] for j in range(nd)], axis=0)

    def wo_copy(l, e):
        slot = lax.rem(e, 2)
        rows = pl.ds(pl.multiple_of(lax.rem(e, hkv) * 2 * dh, 2 * dh), 2 * dh)
        return pltpu.make_async_copy(wo_hbm.at[l, rows], wo.at[slot], wosem.at[slot])

    def rows_of(s):
        return pl.ds(pl.multiple_of(s * r, r), r)

    def norm(s, l):
        g = gs[pl.ds(l, 1), :]

        def blk(rows):
            v = x[rows, :].astype(BF16).astype(F32)
            x[rows, :] = v
            m = lax.rsqrt(jnp.mean(v * v, axis=-1, keepdims=True) + EPS)
            n[rows, :] = (v * m * g).astype(BF16)

        _blocks(s * r, r, blk)

    def out_tiles(s, h, slot, nb):
        rows = rows_of(s)

        def tile(j):
            cols = slice(j * nb, (j + 1) * nb)
            x[rows, cols] += _dot(o[lax.rem(h, 2), rows, :], wo[slot, :, cols])

        return [functools.partial(tile, j) for j in range(d // nb)]

    def out_proj(s, h, slot):
        for tile in out_tiles(s, h, slot, min(512, d)):
            tile()

    def turn(a):
        return _dot_nt(eye[...], a).astype(BF16)

    bar = pltpu.get_barrier_semaphore()
    for nb in (up, down, partner):
        pl.semaphore_signal(bar, inc=1, device_id={'cp': nb}, device_id_type=MESH)
    load_x = pltpu.make_async_copy(x_hbm, n, msem.at[0])
    load_x.start()
    prefetch(KV, 0, 0, nd)

    ro = lax.broadcasted_iota(jnp.int32, (TILE, TILE), 0)
    co = lax.broadcasted_iota(jnp.int32, (TILE, TILE), 1)
    pq[...] = jnp.where(co == (ro % 32) * 8 + ro // 32, 1.0, 0.0).astype(BF16)
    pkv[...] = jnp.where(co == (ro % 32) * 8 + ((ro // 32) % 2) * 4 + ro // 64, 1.0, 0.0).astype(BF16)
    eye[...] = jnp.where(ro == co, 1.0, 0.0).astype(BF16)
    mask[0] = jnp.where(co <= ro, 0.0, NEG).astype(F32)
    mask[1] = jnp.where(co > ro, 0.0, NEG).astype(F32)
    for l in range(nl):
        gs[l:l + 1, :] = g_ref[l:l + 1, :].astype(F32)


    def put_o(s, h, out0, out1):
        rows = rows_of(s)
        o[lax.rem(h, 2), rows, :dh] = out0
        o[lax.rem(h, 2), rows, dh:] = out1

    def attend(s, h, par, fill):
        qi = s * hkv + h
        qv = jnp.concatenate([q[qi, :, :dh], q[qi, :, dh:]], axis=0)
        a = [own(s, h)] + [sl(par, s, p, h) for p in range(4)]
        s0 = _dot_nt(qv, pool[a[0], :, :dh])
        sn = _dot_nt(qv, pool[pl.ds(a[1], 2), :, :dh].reshape(t, dh))
        sf = _dot_nt(qv, pool[pl.ds(a[3], 2), :, :dh].reshape(t, dh))
        miss = [jnp.where((s == 1) | (i >= b), 0.0, NEG).astype(F32) for b in range(5)]
        ch = 64
        probs, inv = [], []
        fill = list(fill)
        steps = 2 * r // ch
        for k in range(steps):
            rows = slice(k * ch, (k + 1) * ch)
            lo = k * ch % r
            sc = [s0[rows] + mask[0, lo:lo + ch, :], sn[rows, :r], sn[rows, r:], sf[rows, :r],
                  sf[rows, r:] + mask[1, lo:lo + ch, :]]
            tops = [jnp.maximum(v[:, :LANES], v[:, LANES:]) for v in sc]
            tops = [tops[0]] + [v + miss[b] for b, v in enumerate(tops) if b]
            m = functools.reduce(jnp.maximum, tops).max(axis=1, keepdims=True) * scale
            pr = [jnp.exp2(v * scale - (m - miss[b])) for b, v in enumerate(sc)]
            inv.append(1.0 / functools.reduce(jnp.add, pr).sum(axis=1, keepdims=True))
            probs.append([v.astype(BF16) for v in pr])
            for _ in range(-(-len(fill) // (steps - k))):
                fill.pop(0)()
        pb = [jnp.concatenate([v[b] for v in probs], axis=0) for b in range(5)]
        num = functools.reduce(jnp.add, [_dot(v, pool[b, :, dh:]) for v, b in zip(pb, a)])
        out = (num * jnp.concatenate(inv, axis=0)).astype(BF16)
        put_o(s, h, out[:r], out[r:])

    def local_send(s, is_lead, h, par):
        start(0, s, h, par)
        if is_lead:
            start(2, s, h, par)
        pl.when(last & (s == 0))(lambda: edge_copy(h, par).start())

    def drain(s, is_lead, h, par):
        for kind in (0, 1, 2, 4) if is_lead else (0, 1, 3, 5):
            pl.when(cond(kind, s))(lambda k=kind: copy(k, s, h, par).wait_send())
        pl.when(last & (s == 0))(lambda: edge_copy(h, par).wait_send())

    def mine(s, k, h):
        return _pick(k, own(s, h), sl(1, s, 1, h), sl(1, s, 3, h), WKV + ((k - 3) * 2 + s) * hh + h * 2)

    def theirs(s, k, h):
        return _pick(k, sl(1, s, 0, h), sl(1, s, 2, h), sl(0, s, 0, h), WKV + ((k - 3) * 2 + s) * hh + h * 2 + 1)

    def has(s, k):
        return jnp.where(s == 0, k < nz, z + k < nz)

    def sends(s, k):
        return jnp.where(s == 0, k < nz - 1, (z + k < nz) & (z > 0))

    def sidx(s, k, h):
        return (s * nz + k) * hkv + h

    def ici(s, k, h):
        return _remote(pool.at[mine(s, k, h)], pool.at[mine(s, k + 1, h)], isend.at[sidx(s, k, h)], irecv.at[sidx(s, k + 1, h)],
                       dev(s))

    def d2d(s, k, h):
        return _remote(pool.at[mine(s, k, h)], pool.at[theirs(s, k, h)], dsend.at[sidx(s, k, h)], drecv.at[sidx(s, k, h)], partner)

    def push(s, k, h):
        pl.when(sends(s, k))(lambda: ici(s, k, h).start())
        pl.when(has(s, k))(lambda: d2d(s, k, h).start())

    def got_ici(s, k, h):
        ref = pool.at[mine(s, k, h)]
        pl.when(has(s, k))(lambda: pltpu.make_async_copy(ref, ref, irecv.at[sidx(s, k, h)]).wait())

    def got_d2d(s, k, h):
        ref = pool.at[theirs(s, k, h)]
        pl.when(has(s, k))(lambda: pltpu.make_async_copy(ref, ref, drecv.at[sidx(s, k, h)]).wait())

    def global_kv(s, h, y):
        pool[own(s, h), :, :dh] = y[:, :dh]
        pool[own(s, h), :, dh:] = turn(y[:, dh:])
        push(s, 0, h)

    roles = ((follow, FOLLOW), (lead, LEAD))

    def local_keys(s, is_lead, par):
        def one(h):
            pool[own(s, h)] = _dot(n[rows_of(s), :], weights(KV, h)).astype(BF16)
            local_send(s, is_lead, h, par)

        _for(hkv, one)

    def global_keys(s):
        _for(hkv, lambda h: global_kv(s, h, _dot(n[rows_of(s), :], weights(KV, h)).astype(BF16)))

    def forward(is_lead, h, l, par):
        s = lead if is_lead else follow
        arrived(s, 1, h, par, need(s, 1))
        if is_lead:
            arrived(follow, 0, h, par, z >= 0)
        pl.when((h == 0) & (l > 0) & cond(1, s))(lambda: pl.semaphore_wait(credit.at[int(is_lead)], 1))
        for kind in (1, 4) if is_lead else (1, 3):
            start(kind, s, h, par)

    def relay_early(h):
        got_ici(follow, 1, h)
        pl.when((h == 0) & sends(follow, 1))(lambda: pl.semaphore_wait(credit.at[0], 1))
        pl.when(sends(follow, 1))(lambda: ici(follow, 1, h).start())

    def give_credit(is_lead, final):
        s = lead if is_lead else follow
        giver = jnp.where(s == 0, final | (z >= 2), jnp.where(final, z + 2 < nz, z + 1 < nz))

        @pl.when(giver)
        def _():
            to = jnp.where(s == 0, down, up)
            pl.semaphore_signal(credit.at[int(is_lead)], inc=1, device_id={'cp': to}, device_id_type=MESH)

    def clear():
        def one(h):
            for p, when in enumerate(((z == 0) & (c == 0), z == 0, (z == 0) | ((z == 1) & (c == 0)), z < 2)):
                for par in range(2 if p < 2 else 1):
                    pl.when(when)(lambda p=p, par=par: pool.__setitem__(sl(par, 0, p, h), jnp.zeros(pool.shape[1:], BF16)))

        _for(hkv, one)

    with jax.named_scope('entry_x'):
        load_x.wait()
        _blocks(0, t, lambda rows: x.__setitem__((rows, slice(None)), n[rows, :].astype(F32)))
        norm(follow, 0)
    with jax.named_scope('entry_kv'):
        relayout(KV, 0, NO, 0, nd)
        prefetch(Q, 0)
        wo_copy(0, 0).start()
        wo_copy(0, 1).start()
    with jax.named_scope('entry_barrier'):
        pl.semaphore_wait(bar, 3)
    with jax.named_scope('entry_keys_f'):
        local_keys(follow, FOLLOW, 0)
    with jax.named_scope('entry_q'):
        relayout(Q, 0, True)
        prefetch(KV, 1)
    with jax.named_scope('entry_keys_l'):
        norm(lead, 0)
        pl.when(z < 2)(clear)
        for h in range(h3):
            forward(FOLLOW, h, 0, 0)
        local_keys(lead, LEAD, 0)
        release(KV)

    def layer(l):
        par = lax.rem(l, 2)
        final = l == nloc - 1

        @pl.when(final & (z == 0))
        def _():
            pl.semaphore_signal(wrap, inc=1, device_id={'cp': down}, device_id_type=MESH)

        with jax.named_scope('relayout_kv'):
            pl.semaphore_wait(freed.at[0], 1)
            relayout(KV, l + 1, True)
            prefetch(Q, l + 1)
        with jax.named_scope('q'):
            shared(Q)

            def q_group(h):
                y = _dot(n[...], weights(Q, h)).astype(BF16)
                for s in STREAMS:
                    q[s * hkv + h] = y[s * r:(s + 1) * r]

            _for(hkv, q_group)
            release(Q)
        with jax.named_scope('forward_a'):
            forward(FOLLOW, h3, l, par)
            forward(LEAD, 0, l, par)
        with jax.named_scope('relayout_q'):
            relayout(Q, l + 1, NO)
            pl.when(l + 2 < nl)(lambda: prefetch(KV, l + 2))
            forward(LEAD, 1, l, par)

        def edge(h):
            for p, core in ((2, 1), (0, 0)):
                @pl.when(last & (c == core))
                def _():
                    arrived(0, p, h, par, z >= 0)
                    pltpu.make_async_copy(pool.at[sl(par, 0, p, h)], pool.at[sl(par, 1, 3, h)], rsem(par, 1, 3, h)).start()

        def gather(s, is_lead, h):
            at_edge = last & (s == 0)
            if not is_lead:
                edge(h)
            arrived(s, 3, h, par, need(s, 2))
            if is_lead:
                arrived(s, 0, h, par, need(s, 1) & ~at_edge)
                arrived(s, 2, h, par, need(s, 2))
            else:
                start(5, s, h, par)
                arrived(s, 2, h, par, need(s, 1) & ~at_edge)

        def use(is_lead, h):
            return h + (hkv if is_lead else 0)

        def next_wo(e):
            wrapped = lax.div(e + 2, hh)
            wo_copy(l + wrapped, e + 2 - hh * wrapped).start()

        def head(s, is_lead, h, first):
            with jax.named_scope('gather'):
                gather(s, is_lead, h)
                if not first:
                    wo_copy(l, use(is_lead, h - 1)).wait()
            with jax.named_scope('attend'):
                attend(s, h, par, [] if first else out_tiles(s, h - 1, lax.rem(h - 1, 2), 256))
            if not first:
                next_wo(use(is_lead, h - 1))

        def heads(s, is_lead, after):
            head(s, is_lead, 0, True)
            after(0)

            def one(j):
                head(s, is_lead, j + 1, False)
                after(j + 1)

            _for(h3, one)

        def tail(s, is_lead):
            with jax.named_scope('out'):
                wo_copy(l, use(is_lead, h3)).wait()
                out_proj(s, h3, h3 % 2)
                next_wo(use(is_lead, h3))
            with jax.named_scope('norm'):
                norm(s, l + 1)
            with jax.named_scope('drain'):
                _for(hkv, lambda h: drain(s, is_lead, h, par))
                if is_lead:
                    pl.when(~final)(lambda: give_credit(is_lead, False))
                else:
                    give_credit(is_lead, final)
            with jax.named_scope('keys'):
                @pl.when(~final)
                def _():
                    local_keys(s, is_lead, 1 - par)

                @pl.when(final)
                def _():
                    if not is_lead:
                        pl.when(last)(lambda: pl.semaphore_wait(wrap, 1))
                    global_keys(s)

        def ahead(h):
            pl.when(~final)(lambda: forward(FOLLOW, h, l + 1, 1 - par))
            pl.when(final)(lambda: relay_early(h))

        def after_f(h):
            @pl.when(h == 1)
            def _():
                forward(LEAD, 2, l, par)
                forward(LEAD, 3, l, par)
                shared(KV)

        def after_l(h):
            pl.when(h == 1)(lambda: ahead(0))
            pl.when(h == 2)(lambda: ahead(1))

        heads(follow, FOLLOW, after_f)
        pl.semaphore_wait(freed.at[1], 1)
        share_all(Q)
        tail(follow, FOLLOW)
        heads(lead, LEAD, after_l)
        ahead(2)
        tail(lead, LEAD)
        pl.when(~final)(lambda: release(KV))

    _for(nloc, layer)

    shared(Q)

    def q_group(h):
        y = _dot(n[...], weights(Q, h)).astype(BF16)
        for s in STREAMS:
            for g in range(2):
                q[s * hkv + h, :, g * r:(g + 1) * r] = turn(y[s * r:(s + 1) * r, g * dh:(g + 1) * dh])

    _for(hkv, q_group)
    for nb in (up, down, partner):
        pl.semaphore_signal(ready, inc=1, device_id={'cp': nb}, device_id_type=MESH)

    def init(j):
        acc[j] = jnp.zeros(acc.shape[1:], F32)
        ml[j, 0:1, :] = jnp.full((1, t), NEG, F32)
        ml[j, 1:2, :] = jnp.zeros((1, t), F32)

    _for(hh, init)
    pl.semaphore_wait(ready, 3)

    def relay(s, k, h):
        got_ici(s, k, h)
        push(s, k, h)

    relay_early(h3)
    _for(hkv, lambda h: pl.when(has(follow, 1))(lambda: d2d(follow, 1, h).start()))
    keys = lax.broadcasted_iota(jnp.int32, (r, t), 0)
    toks = lax.broadcasted_iota(jnp.int32, (r, t), 1) % r

    def flash(qi, a, b, bias=None):
        qt = q[qi]
        sc = _dot(jnp.concatenate([pool[a, :, :dh], pool[b, :, :dh]], axis=0), qt)
        if bias is not None:
            sc = jnp.concatenate([jnp.where(keys <= toks, sc[:r], NEG), sc[r:] + bias], axis=0)
        old = ml[qi, 0:1, :]
        m = jnp.maximum(old, sc.max(axis=0, keepdims=True))
        f = jnp.exp2((old - m) * scale)
        pr = jnp.exp2((sc - m) * scale)
        ml[qi, 0:1, :] = m
        ml[qi, 1:2, :] = ml[qi, 1:2, :] * f + pr.sum(axis=0, keepdims=True)
        pb = pr.astype(BF16)
        acc[qi] = acc[qi] * f + (_dot(pool[a, :, dh:], pb[:r]) + _dot(pool[b, :, dh:], pb[r:]))

    def step(k, h):
        def job(j):
            qs = jnp.where(j < 2, 1, 0)
            ks = jnp.where(j == 1, 1, 0)
            ok = _pick(j, z >= 0, z + k < nz, z - k >= 0)
            pl.when(ok)(lambda: flash(qs * hkv + h, mine(ks, k, h), theirs(ks, k, h)))

        _for(3, job)

    def first(h):
        bias = [jnp.where(c == a, 0.0, NEG).astype(F32) for a in (1, 0)]
        flash(h, mine(0, 0, h), theirs(0, 0, h), bias[0])
        flash(hkv + h, mine(0, 0, h), theirs(0, 0, h))
        flash(hkv + h, mine(1, 0, h), theirs(1, 0, h), bias[1])

    def finish_o(s, h):
        qi = s * hkv + h
        ob = (acc[qi] * (1.0 / ml[qi, 1:2, :])).astype(BF16)
        put_o(s, h, turn(ob[:, :r]), turn(ob[:, r:]))

    def finish(h):
        for s in STREAMS:
            finish_o(s, h)
        wo_copy(nloc, h).wait()
        for s in STREAMS:
            out_proj(s, h, lax.rem(h, 2))
        pl.when(h + 2 < hkv)(lambda: wo_copy(nloc, h + 2).start())

    def put(rows):
        n[rows, :] = x[rows, :].astype(BF16)
        pltpu.make_async_copy(n.at[rows], y_hbm.at[rows], msem.at[0]).start()

    def drain_unit(j):
        k, h = lax.div(j, hkv), lax.rem(j, hkv)
        for s in STREAMS:
            pl.when(sends(s, k))(lambda s=s: ici(s, k, h).wait_send())
            pl.when(has(s, k))(lambda s=s: d2d(s, k, h).wait_send())

    def ready_keys(k, h):
        with jax.named_scope('got'):
            for s in STREAMS:
                got_d2d(s, k, h)

    def unit(u):
        k = lax.div(u, hkv)
        h = lax.rem(u, hkv)
        ready_keys(k, h)
        with jax.named_scope('flash'):
            pl.when(k == 0)(lambda: first(h))
            pl.when(k > 0)(lambda: step(k, h))
        with jax.named_scope('finish'):
            pl.when(k == nz - 1)(lambda: finish(h))
            pl.when(k > 1)(lambda: drain_unit(u - hh))
        pl.when(k == 0)(lambda: relay(lead, 1, h))
        v = u + 1

        @pl.when((v >= hh) & (v < nz * hkv))
        def _():
            for s in STREAMS:
                relay(s, lax.div(v, hkv), lax.rem(v, hkv))

    units = nz * hkv
    with jax.named_scope('units'):
        _for(units - 1, unit)
    _for(hkv + 1, lambda j: drain_unit(units - hh - 1 + j))
    wo_copy(nloc, h3).wait()
    ready_keys(nz - 1, h3)
    with jax.named_scope('flash'):
        step(nz - 1, h3)
    with jax.named_scope('end'):
        for s in STREAMS:
            finish_o(s, h3)
        for s in STREAMS:
            out_proj(s, h3, h3 % 2)
            _blocks(s * r, r, put)
        _for(hkv, lambda j: drain_unit(units - hkv + j))
        pltpu.make_async_copy(n, y_hbm, msem.at[0]).wait()


def solution(mesh):
    cp = mesh.shape['cp']

    def body(x, g, wq, wk, wv, wo):
        t, d = x.shape
        r = t // 2
        nl = g.shape[0]
        hq, dh = wq.shape[2], wq.shape[3]
        hkv = wk.shape[2]
        nz = cp // 2
        assert (hq, hkv, dh, r, W) == (8, 4, 256, 256, 1024)
        wq2 = wq.reshape(nl, d * hq, dh)
        wk2, wv2 = (a.reshape(nl, d, hkv, 2, dh // 2).transpose(0, 1, 3, 2, 4).reshape(nl, d * hkv * 2, dh // 2) for a in (wk, wv))
        wo2 = wo.reshape(nl, hq * dh, d)
        hbm = pl.BlockSpec(memory_space=pl.ANY)
        sems = pltpu.SemaphoreType.DMA
        slots = WKV + 2 * (d // 256) * hkv
        assert slots >= WKV + (nz - 3) * 4 * hkv
        return pl.pallas_call(
            functools.partial(_kernel, cp),
            out_shape=jax.ShapeDtypeStruct((t, d), BF16),
            in_specs=[hbm, pl.BlockSpec(memory_space=pltpu.VMEM), hbm, hbm, hbm, hbm],
            out_specs=hbm,
            scratch_shapes=[
                pltpu.VMEM((t, d), F32),
                pltpu.VMEM((t, d), BF16),
                pltpu.VMEM((2 * hkv, r, 2 * dh), BF16),
                pltpu.VMEM((slots, r, 2 * dh), BF16),
                pltpu.VMEM((2, 2 * dh, d), BF16),
                pltpu.VMEM((STAGES, ROWS, 256), BF16),
                pltpu.VMEM((2, t, 2 * dh), BF16),
                pltpu.VMEM((2 * hkv, dh, 2 * r), F32),
                pltpu.VMEM((2 * hkv, 8, 2 * r), F32),
                pltpu.VMEM((2, r, r), F32),
                pltpu.VMEM((8, d), F32),
                pltpu.VMEM((TILE, TILE), BF16),
                pltpu.VMEM((TILE, TILE), BF16),
                pltpu.VMEM((TILE, TILE), BF16),
                sems((1,)), sems((2 * STAGES,)), sems((2,)), sems((d // 256,)), sems((d // 256,)),
                sems((6 * 2 * hkv,)), sems((hkv,)), sems((2 * 2 * 4 * hkv,)),
                sems((2 * nz * hkv,)), sems((2 * nz * hkv,)), sems((2 * nz * hkv,)), sems((2 * nz * hkv,)),
                pltpu.SemaphoreType.REGULAR((2,)), pltpu.SemaphoreType.REGULAR, pltpu.SemaphoreType.REGULAR,
                pltpu.SemaphoreType.REGULAR((2,)),
            ],
            compiler_params=pltpu.CompilerParams(collective_id=0, has_side_effects=True, vmem_limit_bytes=67043328),
            name='layers',
        )(x, g, wq2, wk2, wv2, wo2)

    spec = P(('dp', 'cp'), None)
    return jax.shard_map(body, mesh=mesh, in_specs=(spec, P(), P(), P(), P(), P()), out_specs=spec, check_vma=False)
```
